8 devices in a mesh: dp: 1 (over z), w: 8 (over y, x, core).
Axes of the slice: x: 2, y: 2, z: 1, core: 2. Of those that a mesh axis runs over, the one named last changes fastest.
Arguments:
- hidden: bfloat16 [1024, 2048], P(('dp', 'w'))
- positions: int32 [1024], P(('dp', 'w'))
- k_cache: bfloat16 [2, 1024, 1, 256, 256], P(None, ('dp', 'w'))
- v_cache: bfloat16 [2, 1024, 1, 256, 256], P(None, ('dp', 'w'))
- attn_norm: float32 [2, 2048], P(None, 'w')
- w_query: bfloat16 [2, 2048, 2048], P(None, 'w')
- w_key: bfloat16 [2, 2048, 256], P(None, 'w')
- w_value: bfloat16 [2, 2048, 256], P(None, 'w')
- w_out: bfloat16 [2, 2048, 2048], P(None, 'w')
- mlp_norm: float32 [2, 2048], P(None, 'w')
- w_gate: bfloat16 [2, 2048, 16384], P(None, 'w')
- w_up: bfloat16 [2, 2048, 16384], P(None, 'w')
- w_down: bfloat16 [2, 16384, 2048], P(None, 'w')
Outputs:
- output 1: bfloat16 [1024, 2048], P(('dp', 'w'))
- output 2: bfloat16 [2, 1024, 1, 256, 256], P(None, ('dp', 'w'))
- output 3: bfloat16 [2, 1024, 1, 256, 256], P(None, ('dp', 'w'))
All inputs are finite; a program needn't handle non-finite values.
Results may differ from the reference program's by a relative error of at most 0.0168836.
Values are sent between devices in bfloat16 or wider.
A program may use at most 1 GiB of HBM per device.

```python
import jax
import jax.numpy as jnp
from jax import lax

D = 2048
HEADS = 8
KV_HEADS = 1
HEAD = 256
FF = 16384
BATCH = 1024
SMAX = 256
LAYERS = 2

EPS = 1e-6
ROPE_BASE = 10000.0
Q_DIM = HEADS * HEAD
KV_DIM = KV_HEADS * HEAD
GROUP = HEADS // KV_HEADS


def setup_inputs(seed: int = 0, part: int = 0) -> dict:
    base_key = jax.random.key(seed)
    part_keys = jax.random.split(jax.random.fold_in(base_key, part), 4)
    shared_keys = jax.random.split(jax.random.fold_in(base_key, 65537), 9)
    hidden = jax.random.normal(part_keys[0], (BATCH, D), jnp.float32).astype(jnp.bfloat16)
    positions = jax.random.randint(part_keys[1], (BATCH,), 0, SMAX, jnp.int32)
    positions = positions.at[0].set(SMAX - 1).at[1].set(0)
    cache_shape = (LAYERS, BATCH, KV_HEADS, SMAX, HEAD)
    k_cache = jax.random.normal(part_keys[2], cache_shape, jnp.float32).astype(jnp.bfloat16)
    v_cache = jax.random.normal(part_keys[3], cache_shape, jnp.float32).astype(jnp.bfloat16)

    def weight(key_w, n_rows, n_cols):
        raw_draw = jax.random.normal(key_w, (LAYERS, n_rows, n_cols), jnp.float32)
        return (raw_draw * n_rows ** -0.5).astype(jnp.bfloat16)

    return {
        "hidden": hidden,
        "positions": positions,
        "k_cache": k_cache,
        "v_cache": v_cache,
        "attn_norm": 0.3 * jax.random.normal(shared_keys[0], (LAYERS, D), jnp.float32),
        "w_query": weight(shared_keys[1], D, Q_DIM),
        "w_key": weight(shared_keys[2], D, KV_DIM),
        "w_value": weight(shared_keys[3], D, KV_DIM),
        "w_out": weight(shared_keys[4], Q_DIM, D),
        "mlp_norm": 0.3 * jax.random.normal(shared_keys[5], (LAYERS, D), jnp.float32),
        "w_gate": weight(shared_keys[6], D, FF),
        "w_up": weight(shared_keys[7], D, FF),
        "w_down": weight(shared_keys[8], FF, D),
    }


def rms_norm(hidden, gain):
    hid_f32 = hidden.astype(jnp.float32)
    mean_sq = jnp.mean(hid_f32 * hid_f32, axis=-1, keepdims=True)
    return (hid_f32 * lax.rsqrt(mean_sq + EPS) * (1.0 + gain)).astype(jnp.bfloat16)


def rope_tables(positions):
    half_dim = HEAD // 2
    inv_freq = ROPE_BASE ** (-2.0 * jnp.arange(half_dim, dtype=jnp.float32) / HEAD)
    angles = positions.astype(jnp.float32)[:, None] * inv_freq[None, :]
    return jnp.cos(angles), jnp.sin(angles)


def apply_rope(vectors, cos_tab, sin_tab):
    half_dim = vectors.shape[-1] // 2
    lead_half = vectors[..., :half_dim]
    tail_half = vectors[..., half_dim:]
    cos_b = cos_tab[:, None, :]
    sin_b = sin_tab[:, None, :]
    return jnp.concatenate([lead_half * cos_b - tail_half * sin_b, tail_half * cos_b + lead_half * sin_b], axis=-1)


def decoder_layer(hidden, params, positions, cos_tab, sin_tab):
    gain_attn, w_query, w_key, w_value, w_out, gain_mlp, w_gate, w_up, w_down, k_layer, v_layer = params
    batch_rows = hidden.shape[0]
    normed = rms_norm(hidden, gain_attn)
    q_proj = jnp.dot(normed, w_query, preferred_element_type=jnp.float32).reshape(batch_rows, HEADS, HEAD)
    k_proj = jnp.dot(normed, w_key, preferred_element_type=jnp.float32).reshape(batch_rows, KV_HEADS, HEAD)
    v_proj = jnp.dot(normed, w_value, preferred_element_type=jnp.float32).reshape(batch_rows, KV_HEADS, HEAD)
    q_rot = (apply_rope(q_proj, cos_tab, sin_tab) * HEAD ** -0.5).astype(jnp.bfloat16)
    q_rot = q_rot.reshape(batch_rows, KV_HEADS, GROUP, HEAD)
    k_rot = apply_rope(k_proj, cos_tab, sin_tab).astype(jnp.bfloat16)
    v_new = v_proj.astype(jnp.bfloat16)
    cache_steps = jnp.arange(SMAX)
    write_mask = (cache_steps[None, :] == positions[:, None])[:, None, :, None]
    k_layer = jnp.where(write_mask, k_rot[:, :, None, :], k_layer)
    v_layer = jnp.where(write_mask, v_new[:, :, None, :], v_layer)
    scores = jnp.einsum("bkge,bkse->bkgs", q_rot.astype(jnp.float32), k_layer.astype(jnp.float32))
    is_valid = cache_steps[None, None, None, :] <= positions[:, None, None, None]
    scores = jnp.where(is_valid, scores, -1e30)
    row_max = jnp.max(scores, axis=-1, keepdims=True)
    attn_prob = jnp.exp(scores - row_max)
    row_sum = jnp.sum(attn_prob, axis=-1, keepdims=True)
    attn_vals = jnp.einsum("bkgs,bkse->bkge", attn_prob.astype(jnp.bfloat16).astype(jnp.float32), v_layer.astype(jnp.float32))
    attn_vals = (attn_vals / row_sum).astype(jnp.bfloat16).reshape(batch_rows, Q_DIM)
    hid_mid = (hidden.astype(jnp.float32) + jnp.dot(attn_vals, w_out, preferred_element_type=jnp.float32)).astype(jnp.bfloat16)
    normed_mlp = rms_norm(hid_mid, gain_mlp)
    gate_pre = jnp.dot(normed_mlp, w_gate, preferred_element_type=jnp.float32)
    up_pre = jnp.dot(normed_mlp, w_up, preferred_element_type=jnp.float32)
    mlp_hidden = (jax.nn.gelu(gate_pre, approximate=True) * up_pre).astype(jnp.bfloat16)
    hid_out = (hid_mid.astype(jnp.float32) + jnp.dot(mlp_hidden, w_down, preferred_element_type=jnp.float32)).astype(jnp.bfloat16)
    return hid_out, (k_layer, v_layer)


def reference(hidden, positions, k_cache, v_cache, attn_norm, w_query, w_key, w_value, w_out, mlp_norm, w_gate, w_up, w_down):
    cos_tab, sin_tab = rope_tables(positions)

    def layer_step(hid_carry, params):
        return decoder_layer(hid_carry, params, positions, cos_tab, sin_tab)

    layer_params = (attn_norm, w_query, w_key, w_value, w_out, mlp_norm, w_gate, w_up, w_down, k_cache, v_cache)
    hidden_out, caches_out = lax.scan(layer_step, hidden, layer_params)
    return hidden_out, caches_out[0], caches_out[1]
```

```python
import jax
import jax.numpy as jnp
from jax import lax
from jax.sharding import PartitionSpec as P

EPS = 1e-6
ROPE_BASE = 10000.0


def rms_norm(hidden, gain):
    hid_f32 = hidden.astype(jnp.float32)
    mean_sq = jnp.mean(hid_f32 * hid_f32, axis=-1, keepdims=True)
    return (hid_f32 * lax.rsqrt(mean_sq + EPS) * (1.0 + gain)).astype(jnp.bfloat16)


def rope_tables(positions, head_dim):
    half_dim = head_dim // 2
    inv_freq = ROPE_BASE ** (-2.0 * jnp.arange(half_dim, dtype=jnp.float32) / head_dim)
    angles = positions.astype(jnp.float32)[:, None] * inv_freq[None, :]
    return jnp.cos(angles), jnp.sin(angles)


def apply_rope(vectors, cos_tab, sin_tab):
    half_dim = vectors.shape[-1] // 2
    lead_half = vectors[..., :half_dim]
    tail_half = vectors[..., half_dim:]
    cos_b = cos_tab[:, None, :]
    sin_b = sin_tab[:, None, :]
    return jnp.concatenate([lead_half * cos_b - tail_half * sin_b, tail_half * cos_b + lead_half * sin_b], axis=-1)


def attention_core(q_proj, k_proj, v_proj, positions, cos_tab, sin_tab, k_layer, v_layer):
    batch_rows, kv_heads, cache_len, head_dim = k_layer.shape
    num_heads = q_proj.shape[-1] // head_dim
    q_rot = apply_rope(q_proj.reshape(batch_rows, num_heads, head_dim), cos_tab, sin_tab)
    q_rot = (q_rot * head_dim ** -0.5).astype(jnp.bfloat16).reshape(batch_rows, kv_heads, num_heads // kv_heads, head_dim)
    k_rot = apply_rope(k_proj.reshape(batch_rows, kv_heads, head_dim), cos_tab, sin_tab).astype(jnp.bfloat16)
    v_new = v_proj.reshape(batch_rows, kv_heads, head_dim).astype(jnp.bfloat16)
    cache_steps = jnp.arange(cache_len)
    write_mask = (cache_steps[None, :] == positions[:, None])[:, None, :, None]
    k_layer = jnp.where(write_mask, k_rot[:, :, None, :], k_layer)
    v_layer = jnp.where(write_mask, v_new[:, :, None, :], v_layer)
    scores = jnp.einsum("bkge,bkse->bkgs", q_rot, k_layer, preferred_element_type=jnp.float32)
    is_valid = cache_steps[None, None, None, :] <= positions[:, None, None, None]
    scores = jnp.where(is_valid, scores, -1e30)
    row_max = jnp.max(scores, axis=-1, keepdims=True)
    attn_prob = jnp.exp(scores - row_max)
    row_sum = jnp.sum(attn_prob, axis=-1, keepdims=True)
    attn_vals = jnp.einsum("bkgs,bkse->bkge", attn_prob.astype(jnp.bfloat16), v_layer, preferred_element_type=jnp.float32)
    attn_vals = (attn_vals / row_sum).astype(jnp.bfloat16).reshape(batch_rows, num_heads * head_dim)
    return attn_vals, k_layer, v_layer


def gather_rows(row_shard):
    return lax.all_gather(row_shard, "w", axis=0, tiled=True)


def exchange_columns(weight_shard, rank, ways):
    rows, cols = weight_shard.shape
    width = cols // ways
    whole = jnp.zeros((rows * ways, width), weight_shard.dtype)
    for mask in range(ways):
        peer = jnp.bitwise_xor(rank, mask)
        block = lax.dynamic_slice(weight_shard, (0, peer * width), (rows, width))
        if mask:
            block = lax.ppermute(block, "w", [(s, s ^ mask) for s in range(ways)])
        whole = lax.dynamic_update_slice(whole, block, (peer * rows, 0))
    return whole


def solution(mesh):
    batch_spec = P(("dp", "w"))
    cache_spec = P(None, ("dp", "w"))
    gain_spec = P(None, "w")
    weight_spec = P(None, "w", None)
    ways = mesh.shape["w"]

    def per_device(hidden, positions, k_cache, v_cache, attn_norm, w_query, w_key, w_value, w_out, mlp_norm, w_gate, w_up, w_down):
        rank = lax.axis_index("w")
        cos_tab, sin_tab = rope_tables(positions, k_cache.shape[-1])
        k_layers = []
        v_layers = []
        for layer_idx in range(k_cache.shape[0]):
            gate_cols = exchange_columns(w_gate[layer_idx], rank, ways)
            up_cols = exchange_columns(w_up[layer_idx], rank, ways)
            normed = rms_norm(hidden, gather_rows(attn_norm[layer_idx]))
            q_proj = jnp.dot(normed, gather_rows(w_query[layer_idx]), preferred_element_type=jnp.float32)
            k_proj = jnp.dot(normed, gather_rows(w_key[layer_idx]), preferred_element_type=jnp.float32)
            v_proj = jnp.dot(normed, gather_rows(w_value[layer_idx]), preferred_element_type=jnp.float32)
            attn_vals, k_layer, v_layer = attention_core(q_proj, k_proj, v_proj, positions, cos_tab, sin_tab, k_cache[layer_idx], v_cache[layer_idx])
            hid_mid = (hidden.astype(jnp.float32) + jnp.dot(attn_vals, gather_rows(w_out[layer_idx]), preferred_element_type=jnp.float32)).astype(jnp.bfloat16)
            normed_mlp = gather_rows(rms_norm(hid_mid, gather_rows(mlp_norm[layer_idx])))
            gate_pre = jnp.dot(normed_mlp, gate_cols, preferred_element_type=jnp.float32)
            up_pre = jnp.dot(normed_mlp, up_cols, preferred_element_type=jnp.float32)
            mlp_hidden = (jax.nn.gelu(gate_pre, approximate=True) * up_pre).astype(jnp.bfloat16)
            partial = jnp.dot(mlp_hidden, w_down[layer_idx], preferred_element_type=jnp.float32)
            mlp_out = lax.psum_scatter(partial, "w", scatter_dimension=0, tiled=True)
            hidden = (hid_mid.astype(jnp.float32) + mlp_out).astype(jnp.bfloat16)
            k_layers.append(k_layer)
            v_layers.append(v_layer)
        return hidden, jnp.stack(k_layers), jnp.stack(v_layers)

    in_specs = (batch_spec, batch_spec, cache_spec, cache_spec, gain_spec, weight_spec, weight_spec, weight_spec, weight_spec, gain_spec, weight_spec, weight_spec, weight_spec)
    out_specs = (batch_spec, cache_spec, cache_spec)
    return jax.shard_map(per_device, mesh=mesh, in_specs=in_specs, out_specs=out_specs, check_vma=False)
```

```python
import functools

import jax
import jax.numpy as jnp
from jax import lax
from jax.experimental import pallas as pl
from jax.experimental.pallas import tpu as pltpu
from jax.sharding import PartitionSpec as P

EPS = 1e-6
ROPE_BASE = 10000.0
MESH = pl.DeviceIdType.MESH
BF16 = jnp.bfloat16
F32 = jnp.float32

WAYS = 8
LAYERS = 2
ROWS = 128
BATCH = ROWS * WAYS
D = 2048
SHARD = D // WAYS
HEADS = 8
HEAD = 256
HALF = HEAD // 2
SMAX = 256
FF_BLOCK = 2048
CHUNK = 256
CHUNKS = FF_BLOCK // CHUNK
GROUP = 8
GROUPS = ROWS // GROUP
SUB = 512
PEERS = (6, 7, 2, 4, 3, 5, 1)
AHEAD = 3


def rope_tables(positions):
    inv_freq = ROPE_BASE ** (-2.0 * jnp.arange(HALF, dtype=F32) / HEAD)
    angles = positions.astype(F32)[:, None] * inv_freq[None, :]
    return jnp.cos(angles), jnp.sin(angles)


def al(index, size):
    return pl.ds(pl.multiple_of(index * size, size), size)


def layers_kernel(hid_in, pos_rep, cos_ref, sin_ref, gains_own, k_cache, v_cache,
                  wq, wk, wv, wo, qx, kx, vx, ox, qy, ky, vy, oy, w_gate, w_up, w_down,
                  hid_out, kn_out, vn_out, qbuf, kbuf, vbuf, obuf, gbuf, ubuf,
                  gains_all, hid, x_act, q_head, q_seq, a_seq, a_flat, kn, vn, kv_k, kv_v, w_tile,
                  y_full, g_tile, u_tile, d_tile, m_act, acc, core_recv, p1a, p1b, p2a, p2b,
                  gain_s, gain_r, fwd_s, fwd_r, rel_s, rel_r, chunk_s, chunk_r, y_s, y_r,
                  rs_s, rs_r, tile_sem, kv_sem, gate_sem, down_sem):
    me = lax.axis_index("w")
    core = lax.rem(me, 2)
    xbit = lax.rem(me // 2, 2)
    ybit = me // 4
    peer = [jnp.bitwise_xor(me, m) for m in range(WAYS)]

    def send(src, dst, m, ssem, rsem):
        return pltpu.make_async_remote_copy(src_ref=src, dst_ref=dst, send_sem=ssem, recv_sem=rsem,
                                            device_id={"w": peer[m]}, device_id_type=MESH)

    barrier = pltpu.get_barrier_semaphore()
    for m in range(1, WAYS):
        pl.semaphore_signal(barrier, inc=1, device_id={"w": peer[m]}, device_id_type=MESH)
    pl.semaphore_wait(barrier, WAYS - 1)

    gain_copies = [send(gains_own, gains_all.at[me], m, gain_s.at[m], gain_r.at[m]) for m in range(1, WAYS)]
    for c in gain_copies:
        c.start()
    gains_all[me] = gains_own[...]

    own = (wq, wk, wv, wo)
    from_x = (qx, kx, vx, ox)
    from_y = (qy, ky, vy, oy)
    bufs = (qbuf, kbuf, vbuf, obuf)
    half = SHARD // 2

    def forwards(l, a):
        return (send(from_x[a].at[l, pl.ds(0, half)], bufs[a].at[l, 6, pl.ds(0, half)], 4, fwd_s.at[l, a, 0], fwd_r.at[l, a, 0]),
                send(from_y[a].at[l, pl.ds(half, half)], bufs[a].at[l, 6, pl.ds(half, half)], 2, fwd_s.at[l, a, 1], fwd_r.at[l, a, 1]))

    def relays(l, a):
        srcs = (own[a].at[l], from_x[a].at[l], from_y[a].at[l], bufs[a].at[l, 6])
        return [send(srcs[i], bufs[a].at[l, 2 * i + 1], 1, rel_s.at[l, a, i], rel_r.at[l, a, i]) for i in range(4)]

    def weights_start(l, a):
        for c in forwards(l, a):
            c.start()
        for c in relays(l, a)[:3]:
            c.start()

    def weights_relay_last(l, a):
        for c in forwards(l, a):
            c.wait_recv()
        relays(l, a)[3].start()

    def weights_arrived(l, a):
        for c in relays(l, a):
            c.wait_recv()

    def chunk_start(g):
        l, k = g // CHUNKS, lax.rem(g, CHUNKS)
        for m in PEERS:
            cols = pl.ds(pl.multiple_of(peer[m] * FF_BLOCK + k * CHUNK, CHUNK), CHUNK)
            send(w_gate.at[l, :, cols], gbuf.at[l, k, al(me, SHARD)], m, chunk_s.at[g, 0], chunk_r.at[g, 0]).start()
            send(w_up.at[l, :, cols], ubuf.at[l, k, al(me, SHARD)], m, chunk_s.at[g, 1], chunk_r.at[g, 1]).start()

    def chunk_wait(sem, g):
        l, k = g // CHUNKS, lax.rem(g, CHUNKS)
        part = pl.ds(0, (WAYS - 1) * SHARD)
        pltpu.make_async_copy(gbuf.at[l, k, part], gbuf.at[l, k, part], sem.at[g, 0]).wait()
        pltpu.make_async_copy(ubuf.at[l, k, part], ubuf.at[l, k, part], sem.at[g, 1]).wait()

    for a in range(4):
        weights_start(0, a)

    @pl.loop(0, AHEAD)
    def _(g):
        chunk_start(g)

    for c in gain_copies:
        c.wait_recv()

    def norm_into(src, gain_row, dst, dst_row0):
        @pl.loop(0, ROWS // 32)
        def _(i):
            h = src[al(i, 32), :].astype(F32)
            r = lax.rsqrt(jnp.mean(h * h, axis=-1, keepdims=True) + EPS)
            for s in range(WAYS):
                cols = pl.ds(s * SHARD, SHARD)
                g = 1.0 + gains_all[s, pl.ds(gain_row, 1), :]
                dst[pl.ds(pl.multiple_of(dst_row0 + i * 32, 32), 32), cols] = (h[:, s * SHARD:(s + 1) * SHARD] * r * g).astype(BF16)

    def tile_copies(l, a, n, slot):
        cols = al(n, HEAD)
        srcs = (own[a].at[l], bufs[a].at[l, 1], from_x[a].at[l], bufs[a].at[l, 3],
                from_y[a].at[l], bufs[a].at[l, 5], bufs[a].at[l, 6], bufs[a].at[l, 7])
        return [pltpu.make_async_copy(srcs[m].at[:, cols], w_tile.at[slot, al(peer[m], SHARD)], tile_sem.at[slot])
                for m in range(WAYS)]

    def tile_start(l, a, n, slot):
        for c in tile_copies(l, a, n, slot):
            c.start()

    def tile_wait(slot):
        pltpu.make_async_copy(w_tile.at[slot], w_tile.at[slot], tile_sem.at[slot]).wait()

    def rope(vec):
        lead, tail = vec[:, :HALF], vec[:, HALF:]
        cos_b, sin_b = cos_ref[...], sin_ref[...]
        return jnp.concatenate([lead * cos_b - tail * sin_b, tail * cos_b + lead * sin_b], axis=-1)

    def kv_copies(l, i, slot):
        return (pltpu.make_async_copy(k_cache.at[l, al(i, GROUP)], kv_k.at[slot], kv_sem.at[slot, 0]),
                pltpu.make_async_copy(v_cache.at[l, al(i, GROUP)], kv_v.at[slot], kv_sem.at[slot, 1]))

    def kv_start(l, i, slot):
        for c in kv_copies(l, i, slot):
            c.start()

    def attention_step(l, i):
        slot = lax.rem(i, 2)

        @pl.when(i + 1 < GROUPS)
        def _():
            kv_start(l, i + 1, 1 - slot)

        for c in kv_copies(l, i, slot):
            c.wait()
        rows = GROUP * HEADS
        q64 = q_seq[al(i, GROUP)].reshape(rows, HEAD)
        kn64 = jnp.broadcast_to(kn[al(i, GROUP), :][:, None, :], (GROUP, HEADS, HEAD)).reshape(rows, HEAD)
        vn64 = jnp.broadcast_to(vn[al(i, GROUP), :][:, None, :], (GROUP, HEADS, HEAD)).reshape(rows, HEAD)
        pos = pos_rep[al(i, rows), :]
        scores = jnp.concatenate(
            [lax.dot_general(q64[s * HEADS:(s + 1) * HEADS].astype(BF16), kv_k[slot, s], (((1,), (1,)), ((), ())), preferred_element_type=F32)
             for s in range(GROUP)], axis=0)
        new_score = jnp.sum(q64 * kn64, axis=-1, keepdims=True)
        place = lax.broadcasted_iota(jnp.int32, (rows, SMAX), 1)
        is_new = place == pos
        scores = jnp.where(is_new, new_score, scores)
        scores = jnp.where(place <= pos, scores, -1e30)
        u = jnp.exp(scores - jnp.max(scores, axis=-1, keepdims=True))
        den = jnp.sum(u, axis=-1, keepdims=True)
        u_new = jnp.sum(jnp.where(is_new, u, 0.0), axis=-1, keepdims=True).astype(BF16).astype(F32)
        u_old = jnp.where(is_new, 0.0, u)
        vals = jnp.concatenate(
            [jnp.dot(u_old[s * HEADS:(s + 1) * HEADS].astype(BF16), kv_v[slot, s], preferred_element_type=F32)
             for s in range(GROUP)], axis=0)
        vals = (vals + u_new * vn64) / den
        a_seq[al(i, GROUP)] = vals.reshape(GROUP, HEADS, HEAD)

    def y_sends(l):
        mine = y_full.at[l, al(me, ROWS)]
        return {m: send(mine, mine, m, y_s.at[l, m], y_r.at[l, m]) for m in (6, 2, 4, 1)}

    def y_relay(l, m):
        block = y_full.at[l, al(peer[m], ROWS)]
        return send(block, block, 1, y_s.at[l, m + 1], y_r.at[l, m + 1])

    def chunk_tiles(l, k):
        copies = []
        own_cols = pl.ds(pl.multiple_of(me * FF_BLOCK + k * CHUNK, CHUNK), CHUNK)
        for w_own, buf, tile, s in ((w_gate, gbuf, g_tile, 0), (w_up, ubuf, u_tile, 1)):
            for m in range(WAYS):
                src = w_own.at[l, :, own_cols] if m == 0 else buf.at[l, k, al(peer[m], SHARD)]
                copies.append(pltpu.make_async_copy(src, tile.at[al(peer[m], SHARD)], gate_sem.at[s]))
        return copies

    def mlp_chunk(l, k, down):
        g = l * CHUNKS + k
        d_copy = pltpu.make_async_copy(w_down.at[l, al(k, CHUNK)], d_tile, down_sem.at[0])
        d_copy.start()
        chunk_wait(chunk_r, g)
        for c in chunk_tiles(l, k):
            c.start()
        pltpu.make_async_copy(g_tile, g_tile, gate_sem.at[0]).wait()
        pltpu.make_async_copy(u_tile, u_tile, gate_sem.at[1]).wait()

        @pl.loop(0, BATCH // 256)
        def _(i):
            y = y_full[l, al(i, 256), :]
            gate = jnp.dot(y, g_tile[...], preferred_element_type=F32)
            up = jnp.dot(y, u_tile[...], preferred_element_type=F32)
            m_act[al(i, 256), :] = (jax.nn.gelu(gate, approximate=True) * up).astype(BF16)

        d_copy.wait()
        down()

    def down_piece(s, first):
        cols = pl.ds(s * SUB, SUB) if isinstance(s, int) else al(s, SUB)

        @pl.loop(0, BATCH // 256)
        def _(i):
            part = jnp.dot(m_act[al(i, 256), :], d_tile[:, cols], preferred_element_type=F32)
            for b in range(256 // ROWS):
                blk = i * (256 // ROWS) + b
                piece = part[b * ROWS:(b + 1) * ROWS]
                acc[blk, :, cols] = piece if first else acc[blk, :, cols] + piece

    def rs_core(s):
        cols = pl.ds(s * SUB, SUB)
        return [send(acc.at[2 * j + 1 - core, :, cols], core_recv.at[j, :, cols], 1, rs_s.at[0, s, j], rs_r.at[0, s, j]) for j in range(4)]

    def rs_first(s):
        cols = pl.ds(s * SUB, SUB)
        if s < 2:
            return [send(acc.at[2 * (2 * t + 1 - xbit) + core, :, cols], p1a.at[t, :, cols], 2, rs_s.at[1, s, t], rs_r.at[1, s, t]) for t in range(2)]
        local = pl.ds((s - 2) * SUB, SUB)
        return [send(acc.at[2 * (2 * (1 - ybit) + t) + core, :, cols], p1b.at[t, :, local], 4, rs_s.at[1, s, t], rs_r.at[1, s, t]) for t in range(2)]

    def rs_second(s):
        cols = pl.ds(s * SUB, SUB)
        if s < 2:
            return [send(acc.at[2 * (2 * (1 - ybit) + xbit) + core, :, cols], p2a.at[:, cols], 4, rs_s.at[2, s, 0], rs_r.at[2, s, 0])]
        local = pl.ds((s - 2) * SUB, SUB)
        return [send(acc.at[2 * (2 * ybit + 1 - xbit) + core, :, cols], p2b.at[:, local], 2, rs_s.at[2, s, 0], rs_r.at[2, s, 0])]

    def rs_core_add(s):
        cols = pl.ds(s * SUB, SUB)
        for c in rs_core(s):
            c.wait_recv()

        @pl.loop(0, 4)
        def _(j):
            acc[2 * j + core, :, cols] = acc[2 * j + core, :, cols] + core_recv[j, :, cols]

    def rs_first_add(s):
        cols = pl.ds(s * SUB, SUB)
        for c in rs_first(s):
            c.wait_recv()

        @pl.loop(0, 2)
        def _(t):
            if s < 2:
                blk = 2 * (2 * t + xbit) + core
                acc[blk, :, cols] = acc[blk, :, cols] + p1a[t, :, cols]
            else:
                blk = 2 * (2 * ybit + t) + core
                acc[blk, :, cols] = acc[blk, :, cols] + p1b[t, :, pl.ds((s - 2) * SUB, SUB)]

    def rs_second_add(s):
        cols = pl.ds(s * SUB, SUB)
        for c in rs_second(s):
            c.wait_recv()
        other = p2a[:, cols] if s < 2 else p2b[:, pl.ds((s - 2) * SUB, SUB)]
        total = acc[me, :, cols] + other
        hid[:, cols] = (hid[:, cols].astype(F32) + total).astype(BF16)

    order = (0, 2, 1, 3)

    hid[...] = hid_in[...]

    for l in range(LAYERS):
        base = l * CHUNKS
        norm_into(hid, l, x_act, 0)
        for a in range(3):
            weights_relay_last(l, a)
        kv_start(l, 0, 0)
        for a in range(3):
            weights_arrived(l, a)
        tile_start(l, 0, 0, 0)

        @pl.loop(0, HEADS)
        def _(h, l=l):
            slot = lax.rem(h, 2)

            @pl.when(h + 1 < HEADS)
            def _():
                tile_start(l, 0, h + 1, 1 - slot)

            tile_wait(slot)
            q = rope(jnp.dot(x_act[...], w_tile[slot], preferred_element_type=F32))
            q_head[h] = (q * HEAD ** -0.5).astype(BF16).astype(F32)

        tile_start(l, 1, 0, 0)
        tile_start(l, 2, 0, 1)
        for h in range(HEADS):
            q_seq[:, h, :] = q_head[h]
        tile_wait(0)
        kn[...] = rope(jnp.dot(x_act[...], w_tile[0], preferred_element_type=F32)).astype(BF16).astype(F32)
        tile_wait(1)
        vn[...] = jnp.dot(x_act[...], w_tile[1], preferred_element_type=F32).astype(BF16).astype(F32)
        kn_out[l] = kn[...].astype(BF16)
        vn_out[l] = vn[...].astype(BF16)

        weights_relay_last(l, 3)
        if l == 1:
            chunk_start(base + 3)

        @pl.loop(0, GROUPS)
        def _(i, l=l):
            attention_step(l, i)

        if l == 1:
            chunk_start(base + 4)
        for h in range(HEADS):
            a_flat[:, pl.ds(h * HEAD, HEAD)] = a_seq[:, h, :].astype(BF16)
        weights_arrived(l, 3)
        tile_start(l, 3, 0, 0)

        @pl.loop(0, HEADS)
        def _(n, l=l):
            slot = lax.rem(n, 2)

            @pl.when(n + 1 < HEADS)
            def _():
                tile_start(l, 3, n + 1, 1 - slot)

            tile_wait(slot)
            cols = al(n, HEAD)
            part = jnp.dot(a_flat[...], w_tile[slot], preferred_element_type=F32)
            hid[:, cols] = (hid[:, cols].astype(F32) + part).astype(BF16)

        norm_into(hid, LAYERS + l, y_full.at[l], me * ROWS)
        ys = y_sends(l)
        for c in ys.values():
            c.start()
        if l == 1:
            chunk_start(base + 5)
        for m in (2, 4, 6):
            ys[m].wait_recv()
            y_relay(l, m).start()
        ys[1].wait_recv()
        for m in (2, 4, 6):
            y_relay(l, m).wait_recv()

        if l == 0:
            for a in range(4):
                weights_start(1, a)

        def start_next(k, l=l):
            nxt = l * CHUNKS + k + (AHEAD if l == 0 else 6)

            @pl.when(nxt < (CHUNKS if l == 0 else 2 * CHUNKS))
            def _():
                chunk_start(nxt)

        def first_down():
            @pl.loop(0, D // SUB)
            def _(s):
                down_piece(s, True)

        def more_down():
            @pl.loop(0, D // SUB)
            def _(s):
                down_piece(s, False)

        start_next(0)
        mlp_chunk(l, 0, first_down)

        @pl.loop(1, CHUNKS - 1)
        def _(k, l=l):
            start_next(k)
            mlp_chunk(l, k, more_down)

        if l == 0:
            chunk_start(CHUNKS)

        def last_down():
            for s in order:
                down_piece(s, False)
                for c in rs_core(s):
                    c.start()

        mlp_chunk(l, CHUNKS - 1, last_down)
        for s in order:
            rs_core_add(s)
            for c in rs_first(s):
                c.start()
        if l == 0:
            chunk_start(CHUNKS + 1)
        for s in order:
            rs_first_add(s)
            for c in rs_second(s):
                c.start()
        if l == 0:
            chunk_start(CHUNKS + 2)
        for s in order:
            rs_second_add(s)
        for s in order:
            for c in rs_core(s) + rs_first(s) + rs_second(s):
                c.wait_send()

    hid_out[...] = hid[...]

    for c in gain_copies:
        c.wait_send()
    for l in range(LAYERS):
        for a in range(4):
            for c in forwards(l, a):
                c.wait_send()
            for c in relays(l, a):
                c.wait_send()
        for c in y_sends(l).values():
            c.wait_send()
        for m in (2, 4, 6):
            y_relay(l, m).wait_send()

    @pl.loop(0, LAYERS * CHUNKS)
    def _(g):
        chunk_wait(chunk_s, g)


def run_layers(*operands):
    any_spec = pl.BlockSpec(memory_space=pl.ANY)
    vmem = pl.BlockSpec(memory_space=pltpu.VMEM)
    sds = jax.ShapeDtypeStruct
    dma = pltpu.SemaphoreType.DMA
    return pl.pallas_call(
        layers_kernel,
        name="layers",
        out_shape=[
            sds((ROWS, D), BF16), sds((LAYERS, ROWS, HEAD), BF16), sds((LAYERS, ROWS, HEAD), BF16),
            sds((LAYERS, WAYS, SHARD, D), BF16), sds((LAYERS, WAYS, SHARD, HEAD), BF16),
            sds((LAYERS, WAYS, SHARD, HEAD), BF16), sds((LAYERS, WAYS, SHARD, D), BF16),
            sds((LAYERS, CHUNKS, D, CHUNK), BF16), sds((LAYERS, CHUNKS, D, CHUNK), BF16),
        ],
        in_specs=[vmem] * 5 + [any_spec] * 17,
        out_specs=[vmem] * 3 + [any_spec] * 6,
        scratch_shapes=[
            pltpu.VMEM((WAYS, 8, SHARD), F32),
            pltpu.VMEM((ROWS, D), BF16),
            pltpu.VMEM((ROWS, D), BF16),
            pltpu.VMEM((HEADS, ROWS, HEAD), F32),
            pltpu.VMEM((ROWS, HEADS, HEAD), F32),
            pltpu.VMEM((ROWS, HEADS, HEAD), F32),
            pltpu.VMEM((ROWS, D), BF16),
            pltpu.VMEM((ROWS, HEAD), F32),
            pltpu.VMEM((ROWS, HEAD), F32),
            pltpu.VMEM((2, GROUP, SMAX, HEAD), BF16),
            pltpu.VMEM((2, GROUP, SMAX, HEAD), BF16),
            pltpu.VMEM((2, D, HEAD), BF16),
            pltpu.VMEM((LAYERS, BATCH, D), BF16),
            pltpu.VMEM((D, CHUNK), BF16),
            pltpu.VMEM((D, CHUNK), BF16),
            pltpu.VMEM((CHUNK, D), BF16),
            pltpu.VMEM((BATCH, CHUNK), BF16),
            pltpu.VMEM((WAYS, ROWS, D), F32),
            pltpu.VMEM((4, ROWS, D), F32),
            pltpu.VMEM((2, ROWS, D // 2), F32),
            pltpu.VMEM((2, ROWS, D // 2), F32),
            pltpu.VMEM((ROWS, D // 2), F32),
            pltpu.VMEM((ROWS, D // 2), F32),
            dma((WAYS,)), dma((WAYS,)),
            dma((LAYERS, 4, 2)), dma((LAYERS, 4, 2)),
            dma((LAYERS, 4, 4)), dma((LAYERS, 4, 4)),
            dma((LAYERS * CHUNKS, 2)), dma((LAYERS * CHUNKS, 2)),
            dma((LAYERS, WAYS)), dma((LAYERS, WAYS)),
            dma((3, 4, 4)), dma((3, 4, 4)),
            dma((2,)), dma((2, 2)), dma((2,)), dma((1,)),
        ],
        compiler_params=pltpu.CompilerParams(collective_id=0, has_side_effects=True, vmem_limit_bytes=60 * 2**20),
        cost_estimate=pl.CostEstimate(flops=60 * 10**9, bytes_accessed=300 * 10**6, transcendentals=0),
    )(*operands)


def copy_kernel(k_in, v_in, k_out, v_out):
    k_out[...] = k_in[...]
    v_out[...] = v_in[...]


def copy_caches(k_cache, v_cache):
    spec = pl.BlockSpec((1, 16, SMAX, HEAD), lambda l, i: (l, i, 0, 0))
    shape = jax.ShapeDtypeStruct(k_cache.shape, k_cache.dtype)
    return pl.pallas_call(
        copy_kernel, name="copy_caches", grid=(LAYERS, ROWS // 16), in_specs=[spec, spec], out_specs=[spec, spec], out_shape=[shape, shape],
        compiler_params=pltpu.CompilerParams(vmem_limit_bytes=40 * 2**20),
        cost_estimate=pl.CostEstimate(flops=20 * 10**9, bytes_accessed=4 * k_cache.size * 2, transcendentals=0),
    )(k_cache, v_cache)


SLAB = 16


def place_kernel(positions, kn, vn, k_in, v_in, k_out, v_out, k_slab, v_slab, sems):
    def slab(ref, l, s):
        base = pl.multiple_of((positions[s] // SLAB) * SLAB, SLAB)
        return ref.at[l, s, pl.ds(base, SLAB), :]

    for l in range(LAYERS):
        @pl.loop(0, ROWS)
        def _(s, l=l):
            pltpu.make_async_copy(slab(k_out, l, s), k_slab.at[l, s], sems.at[0]).start()
            pltpu.make_async_copy(slab(v_out, l, s), v_slab.at[l, s], sems.at[1]).start()

    pltpu.make_async_copy(k_slab, k_slab, sems.at[0]).wait()
    pltpu.make_async_copy(v_slab, v_slab, sems.at[1]).wait()
    row = lax.broadcasted_iota(jnp.int32, (SLAB, HEAD), 0)
    for l in range(LAYERS):
        @pl.loop(0, ROWS // 8)
        def _(i, l=l):
            k8 = kn[l, al(i, 8), :].astype(F32)
            v8 = vn[l, al(i, 8), :].astype(F32)
            for j in range(8):
                s = i * 8 + j
                hit = row == lax.rem(positions[s], SLAB)
                k_slab[l, s] = jnp.where(hit, k8[j:j + 1], k_slab[l, s].astype(F32)).astype(BF16)
                v_slab[l, s] = jnp.where(hit, v8[j:j + 1], v_slab[l, s].astype(F32)).astype(BF16)

    for l in range(LAYERS):
        @pl.loop(0, ROWS)
        def _(s, l=l):
            pltpu.make_async_copy(k_slab.at[l, s], slab(k_out, l, s), sems.at[2]).start()
            pltpu.make_async_copy(v_slab.at[l, s], slab(v_out, l, s), sems.at[3]).start()

    pltpu.make_async_copy(k_slab, k_slab, sems.at[2]).wait()
    pltpu.make_async_copy(v_slab, v_slab, sems.at[3]).wait()


def place_rows(positions, kn, vn, k_copy, v_copy):
    any_spec = pl.BlockSpec(memory_space=pl.ANY)
    vmem = pl.BlockSpec(memory_space=pltpu.VMEM)
    shape = jax.ShapeDtypeStruct(k_copy.shape, k_copy.dtype)
    return pl.pallas_call(
        place_kernel, name="place_rows",
        in_specs=[pl.BlockSpec(memory_space=pltpu.SMEM), vmem, vmem, any_spec, any_spec],
        out_specs=[any_spec, any_spec], out_shape=[shape, shape], input_output_aliases={3: 0, 4: 1},
        scratch_shapes=[pltpu.VMEM((LAYERS, ROWS, SLAB, HEAD), BF16), pltpu.VMEM((LAYERS, ROWS, SLAB, HEAD), BF16), pltpu.SemaphoreType.DMA((4,))],
        compiler_params=pltpu.CompilerParams(vmem_limit_bytes=40 * 2**20),
    )(positions, kn, vn, k_copy, v_copy)


def solution(mesh):
    batch_spec = P(("dp", "w"))
    cache_spec = P(None, ("dp", "w"))
    gain_spec = P(None, "w")
    weight_spec = P(None, "w", None)
    x_swap = [(s, s ^ 2) for s in range(WAYS)]
    y_swap = [(s, s ^ 4) for s in range(WAYS)]

    def per_device(hidden, positions, k_cache, v_cache, attn_norm, w_query, w_key, w_value, w_out, mlp_norm, w_gate, w_up, w_down):
        attn_weights = (w_query, w_key, w_value, w_out)
        from_x = tuple(lax.ppermute(w, "w", x_swap) for w in attn_weights)
        from_y = tuple(lax.ppermute(w, "w", y_swap) for w in attn_weights)
        k_copy, v_copy = copy_caches(k_cache[:, :, 0], v_cache[:, :, 0])
        cos_tab, sin_tab = rope_tables(positions)
        pos_rep = jnp.repeat(positions, HEADS)[:, None]
        gains = jnp.concatenate([attn_norm, mlp_norm, attn_norm, mlp_norm], axis=0)
        outs = run_layers(hidden, pos_rep, cos_tab, sin_tab, gains, k_copy, v_copy, *attn_weights, *from_x, *from_y, w_gate, w_up, w_down)
        hidden_out, k_new, v_new = outs[:3]
        k_out, v_out = place_rows(positions, k_new, v_new, k_copy, v_copy)
        return hidden_out, k_out[:, :, None], v_out[:, :, None]

    in_specs = (batch_spec, batch_spec, cache_spec, cache_spec, gain_spec, weight_spec, weight_spec, weight_spec, weight_spec, gain_spec, weight_spec, weight_spec, weight_spec)
    out_specs = (batch_spec, cache_spec, cache_spec)
    return jax.shard_map(per_device, mesh=mesh, in_specs=in_specs, out_specs=out_specs, check_vma=False)
```

```python
import jax
import jax.numpy as jnp
from jax import lax
from jax.experimental import pallas as pl
from jax.experimental.pallas import tpu as pltpu
from jax.sharding import PartitionSpec as P

EPS = 1e-6
ROPE_BASE = 10000.0
MESH = pl.DeviceIdType.MESH
BF16 = jnp.bfloat16
F32 = jnp.float32

WAYS = 8
LAYERS = 2
ROWS = 128
BATCH = ROWS * WAYS
D = 2048
SHARD = D // WAYS
HEADS = 8
HEAD = 256
HALF = HEAD // 2
SMAX = 256
FF_BLOCK = 2048
CHUNK = 256
CHUNKS = FF_BLOCK // CHUNK
GROUP = 8
GROUPS = ROWS // GROUP
SUB = 512
PIECES = ((0, 256), (1024, 256), (256, 512), (1280, 512), (768, 256), (1792, 256))
SLAB = 16
PEERS = (6, 7, 2, 4, 3, 5, 1)
AHEAD = 2
MROWS = 512
DROWS = 512


def rope_tables(positions):
    inv_freq = ROPE_BASE ** (-2.0 * jnp.arange(HALF, dtype=F32) / HEAD)
    angles = positions.astype(F32)[:, None] * inv_freq[None, :]
    return jnp.cos(angles), jnp.sin(angles)


def al(index, size):
    return pl.ds(pl.multiple_of(index * size, size), size)


def layers_kernel(hid_in, pos_rep, cos_ref, sin_ref, gains_own, k_cache, v_cache, k_slabs, v_slabs,
                  wq, wk, wv, wo, qx, kx, vx, ox, qy, ky, vy, oy, w_gate, w_up, w_down,
                  hid_out, k_slabs_out, v_slabs_out, qbuf, kbuf, vbuf, obuf, gbuf, ubuf,
                  gains_all, hid, x_act, q_head, q_seq, a_seq, a_flat, kn, vn, kv_k, kv_v, w_tile,
                  y_full, g_tile, u_tile, gate_act, d_tile, m_act, acc, core_recv, p1a, p1b, p2a, p2b, k_slab, v_slab, u_last,
                  gain_s, gain_r, fwd_s, fwd_r, rel_s, rel_r, chunk_s, chunk_r, y_s, y_r,
                  rs_s, rs_r, tile_sem, kv_sem, gate_sem, down_sem, slab_sem):
    me = lax.axis_index("w")
    core = lax.rem(me, 2)
    xbit = lax.rem(me // 2, 2)
    ybit = me // 4
    peer = [jnp.bitwise_xor(me, m) for m in range(WAYS)]

    def send(src, dst, m, ssem, rsem):
        return pltpu.make_async_remote_copy(src_ref=src, dst_ref=dst, send_sem=ssem, recv_sem=rsem,
                                            device_id={"w": peer[m]}, device_id_type=MESH)

    barrier = pltpu.get_barrier_semaphore()
    for m in range(1, WAYS):
        pl.semaphore_signal(barrier, inc=1, device_id={"w": peer[m]}, device_id_type=MESH)
    pl.semaphore_wait(barrier, WAYS - 1)

    own = (wq, wk, wv, wo)
    from_x = (qx, kx, vx, ox)
    from_y = (qy, ky, vy, oy)
    bufs = (qbuf, kbuf, vbuf, obuf)
    half = SHARD // 2

    def forwards(l, a):
        return (send(from_x[a].at[l, pl.ds(0, half)], bufs[a].at[l, 6, pl.ds(0, half)], 4, fwd_s.at[l, a, 0], fwd_r.at[l, a, 0]),
                send(from_y[a].at[l, pl.ds(half, half)], bufs[a].at[l, 6, pl.ds(half, half)], 2, fwd_s.at[l, a, 1], fwd_r.at[l, a, 1]))

    def relay(l, a, i):
        src = (own[a], from_x[a], from_y[a])[i].at[l] if i < 3 else bufs[a].at[l, 6]
        return send(src, bufs[a].at[l, 2 * i + 1], 1, rel_s.at[l, a, i], rel_r.at[l, a, i])

    def weights_start(l):
        for a in range(4):
            for c in forwards(l, a):
                c.start()
        for a in range(4):
            for i in range(3):
                relay(l, a, i).start()

    def weights_relay_last(l, a):
        for c in forwards(l, a):
            c.wait_recv()
        relay(l, a, 3).start()

    def weights_arrived(l, a):
        for i in range(4):
            relay(l, a, i).wait_recv()

    ffw = (w_gate, w_up)
    ffbuf = (gbuf, ubuf)

    def unit_start(g, s):
        l, k = g // CHUNKS, lax.rem(g, CHUNKS)
        for m in PEERS:
            cols = pl.ds(pl.multiple_of(peer[m] * FF_BLOCK + k * CHUNK, CHUNK), CHUNK)
            send(ffw[s].at[l, :, cols], ffbuf[s].at[l, k, al(me, SHARD)], m, chunk_s.at[g, s], chunk_r.at[g, s]).start()

    last_g = LAYERS * CHUNKS - 1
    last_own = pltpu.make_async_copy(
        w_up.at[LAYERS - 1, :, pl.ds(pl.multiple_of(me * FF_BLOCK + (CHUNKS - 1) * CHUNK, CHUNK), CHUNK)], u_last.at[al(me, SHARD)], down_sem.at[1])
    last_own.start()

    def last_up_start():
        for m in PEERS:
            cols = pl.ds(pl.multiple_of(peer[m] * FF_BLOCK + (CHUNKS - 1) * CHUNK, CHUNK), CHUNK)
            send(w_up.at[LAYERS - 1, :, cols], u_last.at[al(me, SHARD)], m, chunk_s.at[last_g, 1], chunk_r.at[last_g, 1]).start()

    def last_up_wait():
        last_own.wait()
        part = u_last.at[pl.ds(0, (WAYS - 1) * SHARD)]
        pltpu.make_async_copy(part, part, chunk_r.at[last_g, 1]).wait()

    def unit_wait(sem, g, s):
        l, k = g // CHUNKS, lax.rem(g, CHUNKS)
        part = ffbuf[s].at[l, k, pl.ds(0, (WAYS - 1) * SHARD)]
        pltpu.make_async_copy(part, part, sem.at[g, s]).wait()

    weights_start(0)

    gain_copies = [send(gains_own, gains_all.at[me], m, gain_s.at[m], gain_r.at[m]) for m in range(1, WAYS)]
    for c in gain_copies:
        c.start()
    gains_all[me] = gains_own[...]

    @pl.loop(0, AHEAD)
    def _(g):
        unit_start(g, 0)
        unit_start(g, 1)

    for c in gain_copies:
        c.wait_recv()

    def norm_into(src, gain_row, dst, dst_row0):
        @pl.loop(0, ROWS // 32)
        def _(i):
            h = src[al(i, 32), :].astype(F32)
            r = lax.rsqrt(jnp.mean(h * h, axis=-1, keepdims=True) + EPS)
            for s in range(WAYS):
                cols = pl.ds(s * SHARD, SHARD)
                g = 1.0 + gains_all[s, pl.ds(gain_row, 1), :]
                dst[pl.ds(pl.multiple_of(dst_row0 + i * 32, 32), 32), cols] = (h[:, s * SHARD:(s + 1) * SHARD] * r * g).astype(BF16)

    def tile_copies(l, a, n, slot):
        cols = al(n, HEAD)
        srcs = (own[a].at[l], bufs[a].at[l, 1], from_x[a].at[l], bufs[a].at[l, 3],
                from_y[a].at[l], bufs[a].at[l, 5], bufs[a].at[l, 6], bufs[a].at[l, 7])
        return [pltpu.make_async_copy(srcs[m].at[:, cols], w_tile.at[slot, al(peer[m], SHARD)], tile_sem.at[slot])
                for m in range(WAYS)]

    def tile_start(l, a, n, slot):
        for c in tile_copies(l, a, n, slot):
            c.start()

    def tile_wait(slot):
        pltpu.make_async_copy(w_tile.at[slot], w_tile.at[slot], tile_sem.at[slot]).wait()

    def rope(vec):
        lead, tail = vec[:, :HALF], vec[:, HALF:]
        cos_b, sin_b = cos_ref[...], sin_ref[...]
        return jnp.concatenate([lead * cos_b - tail * sin_b, tail * cos_b + lead * sin_b], axis=-1)

    def kv_copies(l, i, slot):
        return (pltpu.make_async_copy(k_cache.at[l, al(i, GROUP)], kv_k.at[slot], kv_sem.at[slot, 0]),
                pltpu.make_async_copy(v_cache.at[l, al(i, GROUP)], kv_v.at[slot], kv_sem.at[slot, 1]))

    def kv_start(l, i, slot):
        for c in kv_copies(l, i, slot):
            c.start()

    def attention_step(l, i):
        slot = lax.rem(i, 2)

        @pl.when(i + 1 < GROUPS)
        def _():
            kv_start(l, i + 1, 1 - slot)

        for c in kv_copies(l, i, slot):
            c.wait()
        rows = GROUP * HEADS
        q64 = q_seq[al(i, GROUP)].reshape(rows, HEAD)
        kn64 = jnp.broadcast_to(kn[al(i, GROUP), :][:, None, :], (GROUP, HEADS, HEAD)).reshape(rows, HEAD)
        vn64 = jnp.broadcast_to(vn[al(i, GROUP), :][:, None, :], (GROUP, HEADS, HEAD)).reshape(rows, HEAD)
        pos = pos_rep[al(i, rows), :]
        scores = jnp.concatenate(
            [lax.dot_general(q64[s * HEADS:(s + 1) * HEADS].astype(BF16), kv_k[slot, s], (((1,), (1,)), ((), ())), preferred_element_type=F32)
             for s in range(GROUP)], axis=0)
        new_score = jnp.sum(q64 * kn64, axis=-1, keepdims=True)
        place = lax.broadcasted_iota(jnp.int32, (rows, SMAX), 1)
        is_new = place == pos
        scores = jnp.where(is_new, new_score, scores)
        scores = jnp.where(place <= pos, scores, -1e30)
        u = jnp.exp(scores - jnp.max(scores, axis=-1, keepdims=True))
        den = jnp.sum(u, axis=-1, keepdims=True)
        u_new = jnp.sum(jnp.where(is_new, u, 0.0), axis=-1, keepdims=True).astype(BF16).astype(F32)
        u_old = jnp.where(is_new, 0.0, u)
        vals = jnp.concatenate(
            [jnp.dot(u_old[s * HEADS:(s + 1) * HEADS].astype(BF16), kv_v[slot, s], preferred_element_type=F32)
             for s in range(GROUP)], axis=0)
        vals = (vals + u_new * vn64) / den
        a_seq[al(i, GROUP)] = vals.reshape(GROUP, HEADS, HEAD)

    def y_send(l, m):
        mine = y_full.at[l, al(me, ROWS)]
        return send(mine, mine, m, y_s.at[l, m], y_r.at[l, m])

    def y_forward(l, m):
        first = 0 if m == 2 else ROWS // 2
        block = y_full.at[l, pl.ds(pl.multiple_of(peer[m] * ROWS + first, ROWS // 2), ROWS // 2)]
        i = 6 if m == 2 else 0
        return send(block, block, 6 - m, y_s.at[l, i], y_r.at[l, i])

    def y_relay(l, m):
        block = y_full.at[l, al(peer[m], ROWS)]
        return send(block, block, 1, y_s.at[l, m + 1], y_r.at[l, m + 1])

    fftile = (g_tile, u_tile)

    def tile_in(l, k, s):
        unit_wait(chunk_r, l * CHUNKS + k, s)
        slot = lax.rem(k, 2)
        own_cols = pl.ds(pl.multiple_of(me * FF_BLOCK + k * CHUNK, CHUNK), CHUNK)
        for m in range(WAYS):
            src = ffw[s].at[l, :, own_cols] if m == 0 else ffbuf[s].at[l, k, al(peer[m], SHARD)]
            pltpu.make_async_copy(src, fftile[s].at[slot, al(peer[m], SHARD)], gate_sem.at[s, slot]).start()

    def tile_ready(k, s):
        slot = lax.rem(k, 2)
        pltpu.make_async_copy(fftile[s].at[slot], fftile[s].at[slot], gate_sem.at[s, slot]).wait()

    def mlp_chunk(l, k, last, down):
        slot = lax.rem(k, 2)
        d_copy = pltpu.make_async_copy(w_down.at[l, al(k, CHUNK)], d_tile, down_sem.at[0])
        d_copy.start()
        tile_ready(k, 0)
        if not last:
            tile_in(l, k, 1)

        @pl.loop(0, BATCH // MROWS)
        def _(i):
            gate = jnp.dot(y_full[l, al(i, MROWS), :], g_tile[slot], preferred_element_type=F32)
            gate_act[al(i, MROWS), :] = jax.nn.gelu(gate, approximate=True)

        direct = last and l == LAYERS - 1
        if direct:
            last_up_wait()
        else:
            if last:
                tile_in(l, k, 1)
            tile_ready(k, 1)

        @pl.loop(0, BATCH // MROWS)
        def _(i):
            u_cols = u_last[...] if direct else u_tile[slot]
            up = jnp.dot(y_full[l, al(i, MROWS), :], u_cols, preferred_element_type=F32)
            m_act[al(i, MROWS), :] = (gate_act[al(i, MROWS), :] * up).astype(BF16)

        if not last:
            tile_in(l, k + 1, 0)
        d_copy.wait()
        down()

    def down_piece(cols, first):
        @pl.loop(0, BATCH // DROWS)
        def _(i):
            part = jnp.dot(m_act[al(i, DROWS), :], d_tile[:, cols], preferred_element_type=F32)
            for b in range(DROWS // ROWS):
                blk = i * (DROWS // ROWS) + b
                piece = part[b * ROWS:(b + 1) * ROWS]
                acc[blk, :, cols] = piece if first else acc[blk, :, cols] + piece

    half_d = D // 2

    def piece(s):
        start, width = PIECES[s]
        return start < half_d, pl.ds(start, width), pl.ds(start % half_d, width)

    def rs_core(s):
        _, cols, _ = piece(s)
        return [send(acc.at[2 * j + 1 - core, :, cols], core_recv.at[j, :, cols], 1, rs_s.at[0, s, j], rs_r.at[0, s, j]) for j in range(4)]

    def rs_first(s):
        left, cols, local = piece(s)
        if left:
            return [send(acc.at[2 * (2 * t + 1 - xbit) + core, :, cols], p1a.at[t, :, local], 2, rs_s.at[1, s, t], rs_r.at[1, s, t]) for t in range(2)]
        return [send(acc.at[2 * (2 * (1 - ybit) + t) + core, :, cols], p1b.at[t, :, local], 4, rs_s.at[1, s, t], rs_r.at[1, s, t]) for t in range(2)]

    def rs_second(s):
        left, cols, local = piece(s)
        if left:
            return [send(acc.at[2 * (2 * (1 - ybit) + xbit) + core, :, cols], p2a.at[:, local], 4, rs_s.at[2, s, 0], rs_r.at[2, s, 0])]
        return [send(acc.at[2 * (2 * ybit + 1 - xbit) + core, :, cols], p2b.at[:, local], 2, rs_s.at[2, s, 0], rs_r.at[2, s, 0])]

    def rs_core_add(s):
        _, cols, _ = piece(s)
        for c in rs_core(s):
            c.wait_recv()

        @pl.loop(0, 4)
        def _(j):
            acc[2 * j + core, :, cols] = acc[2 * j + core, :, cols] + core_recv[j, :, cols]

    def rs_first_add(s):
        left, cols, local = piece(s)
        for c in rs_first(s):
            c.wait_recv()

        @pl.loop(0, 2)
        def _(t):
            if left:
                blk = 2 * (2 * t + xbit) + core
                acc[blk, :, cols] = acc[blk, :, cols] + p1a[t, :, local]
            else:
                blk = 2 * (2 * ybit + t) + core
                acc[blk, :, cols] = acc[blk, :, cols] + p1b[t, :, local]

    def rs_second_add(s):
        left, cols, local = piece(s)
        for c in rs_second(s):
            c.wait_recv()
        other = p2a[:, local] if left else p2b[:, local]
        total = acc[me, :, cols] + other
        hid[:, cols] = (hid[:, cols].astype(F32) + total).astype(BF16)

    def slab_in(l):
        return (pltpu.make_async_copy(k_slabs.at[l], k_slab.at[l], slab_sem.at[l, 0]),
                pltpu.make_async_copy(v_slabs.at[l], v_slab.at[l], slab_sem.at[l, 1]))

    def slab_out(l):
        return (pltpu.make_async_copy(k_slab.at[l], k_slabs_out.at[l], slab_sem.at[l, 2]),
                pltpu.make_async_copy(v_slab.at[l], v_slabs_out.at[l], slab_sem.at[l, 3]))

    def slab_fill(l):
        for c in slab_in(l):
            c.wait()
        row = lax.broadcasted_iota(jnp.int32, (SLAB, HEAD), 0)

        @pl.loop(0, GROUPS)
        def _(i):
            k8 = kn[al(i, GROUP), :]
            v8 = vn[al(i, GROUP), :]
            pos = pos_rep[al(i, GROUP * HEADS), :]
            for j in range(GROUP):
                q = i * GROUP + j
                hit = row == jnp.bitwise_and(pos[j * HEADS:j * HEADS + 1], SLAB - 1)
                k_slab[l, q] = jnp.where(hit, k8[j:j + 1], k_slab[l, q].astype(F32)).astype(BF16)
                v_slab[l, q] = jnp.where(hit, v8[j:j + 1], v_slab[l, q].astype(F32)).astype(BF16)

        for c in slab_out(l):
            c.start()

    order = range(len(PIECES))
    for l in range(LAYERS):
        for c in slab_in(l):
            c.start()

    hid[...] = hid_in[...]

    for l in range(LAYERS):
        base = l * CHUNKS
        norm_into(hid, l, x_act, 0)
        if l == 0:
            for a in range(3):
                weights_relay_last(l, a)
        kv_start(l, 0, 0)
        for a in range(3):
            weights_arrived(l, a)
        tile_start(l, 0, 0, 0)

        @pl.loop(0, HEADS)
        def _(h, l=l):
            slot = lax.rem(h, 2)

            @pl.when(h + 1 < HEADS)
            def _():
                tile_start(l, 0, h + 1, 1 - slot)

            tile_wait(slot)
            q = rope(jnp.dot(x_act[...], w_tile[slot], preferred_element_type=F32))
            q_head[h] = (q * HEAD ** -0.5).astype(BF16).astype(F32)

        tile_start(l, 1, 0, 0)
        tile_start(l, 2, 0, 1)
        for h in range(HEADS):
            q_seq[:, h, :] = q_head[h]
        tile_wait(0)
        kn[...] = rope(jnp.dot(x_act[...], w_tile[0], preferred_element_type=F32)).astype(BF16).astype(F32)
        tile_wait(1)
        vn[...] = jnp.dot(x_act[...], w_tile[1], preferred_element_type=F32).astype(BF16).astype(F32)

        if l == 0:
            weights_relay_last(l, 3)
        else:
            unit_start(base + 1, 1)

        @pl.loop(0, GROUPS // 2)
        def _(i, l=l):
            attention_step(l, i)

        unit_start(base + 2, 0)

        @pl.loop(GROUPS // 2, GROUPS)
        def _(i, l=l):
            attention_step(l, i)

        if l == 0:
            unit_start(base + 2, 1)
        for h in range(HEADS):
            a_flat[:, pl.ds(h * HEAD, HEAD)] = a_seq[:, h, :].astype(BF16)
        weights_arrived(l, 3)
        tile_start(l, 3, 0, 0)

        @pl.loop(0, HEADS)
        def _(n, l=l):
            slot = lax.rem(n, 2)

            @pl.when(n + 1 < HEADS)
            def _():
                tile_start(l, 3, n + 1, 1 - slot)

            tile_wait(slot)
            cols = al(n, HEAD)
            part = jnp.dot(a_flat[...], w_tile[slot], preferred_element_type=F32)
            hid[:, cols] = (hid[:, cols].astype(F32) + part).astype(BF16)

        norm_into(hid, LAYERS + l, y_full.at[l], me * ROWS)
        for m in (2, 4, 1):
            y_send(l, m).start()
        if l == 0:
            unit_start(base + 3, 0)
        for m in (2, 4):
            y_send(l, m).wait_recv()
            y_forward(l, m).start()
        if l == 1:
            unit_start(base + 2, 1)
            unit_start(base + 3, 0)
        unit_start(base + 3, 1)
        for m in (2, 4):
            y_relay(l, m).start()
        for m in (2, 4):
            y_forward(l, m).wait_recv()
        y_relay(l, 6).start()
        y_send(l, 1).wait_recv()
        for m in (2, 4, 6):
            y_relay(l, m).wait_recv()

        if l == 0:
            weights_start(1)

        @pl.loop(base + 4, base + CHUNKS - l)
        def _(g):
            unit_start(g, 0)
            unit_start(g, 1)

        if l == LAYERS - 1:
            unit_start(last_g, 0)
            last_up_start()

        def first_down():
            @pl.loop(0, D // SUB)
            def _(s):
                down_piece(al(s, SUB), True)

        def more_down():
            @pl.loop(0, D // SUB)
            def _(s):
                down_piece(al(s, SUB), False)

        tile_in(l, 0, 0)
        mlp_chunk(l, 0, False, first_down)

        @pl.loop(1, CHUNKS - 1)
        def _(k, l=l):
            mlp_chunk(l, k, False, more_down)

        if l == 0:
            for a in range(4):
                weights_relay_last(1, a)
            unit_start(CHUNKS, 0)

        def last_down():
            for s in order:
                down_piece(pl.ds(*PIECES[s]), False)
                for c in rs_core(s):
                    c.start()

        mlp_chunk(l, CHUNKS - 1, True, last_down)
        for s in order:
            rs_core_add(s)
            for c in rs_first(s):
                c.start()
        slab_fill(l)
        for s in order:
            rs_first_add(s)
            for c in rs_second(s):
                c.start()
        if l == 0:
            unit_start(CHUNKS, 1)
            unit_start(CHUNKS + 1, 0)
        for s in order:
            rs_second_add(s)
        for s in order:
            for c in rs_core(s) + rs_first(s) + rs_second(s):
                c.wait_send()

    hid_out[...] = hid[...]

    for c in gain_copies:
        c.wait_send()
    for l in range(LAYERS):
        for c in slab_out(l):
            c.wait()
        for a in range(4):
            for c in forwards(l, a):
                c.wait_send()
            for i in range(4):
                relay(l, a, i).wait_send()
        for m in (2, 4, 1):
            y_send(l, m).wait_send()
        for m in (2, 4):
            y_forward(l, m).wait_send()
        for m in (2, 4, 6):
            y_relay(l, m).wait_send()

    @pl.loop(0, LAYERS * CHUNKS)
    def _(g):
        unit_wait(chunk_s, g, 0)
        unit_wait(chunk_s, g, 1)


def run_layers(*operands):
    any_spec = pl.BlockSpec(memory_space=pl.ANY)
    vmem = pl.BlockSpec(memory_space=pltpu.VMEM)
    sds = jax.ShapeDtypeStruct
    dma = pltpu.SemaphoreType.DMA
    return pl.pallas_call(
        layers_kernel,
        name="layers",
        out_shape=[
            sds((ROWS, D), BF16), sds((LAYERS, ROWS, SLAB, HEAD), BF16), sds((LAYERS, ROWS, SLAB, HEAD), BF16),
            sds((LAYERS, WAYS, SHARD, D), BF16), sds((LAYERS, WAYS, SHARD, HEAD), BF16),
            sds((LAYERS, WAYS, SHARD, HEAD), BF16), sds((LAYERS, WAYS, SHARD, D), BF16),
            sds((LAYERS, CHUNKS, D, CHUNK), BF16), sds((LAYERS, CHUNKS, D, CHUNK), BF16),
        ],
        in_specs=[vmem] * 5 + [any_spec] * 19,
        out_specs=[vmem] + [any_spec] * 8,
        scratch_shapes=[
            pltpu.VMEM((WAYS, 8, SHARD), F32),
            pltpu.VMEM((ROWS, D), BF16),
            pltpu.VMEM((ROWS, D), BF16),
            pltpu.VMEM((HEADS, ROWS, HEAD), F32),
            pltpu.VMEM((ROWS, HEADS, HEAD), F32),
            pltpu.VMEM((ROWS, HEADS, HEAD), F32),
            pltpu.VMEM((ROWS, D), BF16),
            pltpu.VMEM((ROWS, HEAD), F32),
            pltpu.VMEM((ROWS, HEAD), F32),
            pltpu.VMEM((2, GROUP, SMAX, HEAD), BF16),
            pltpu.VMEM((2, GROUP, SMAX, HEAD), BF16),
            pltpu.VMEM((2, D, HEAD), BF16),
            pltpu.VMEM((LAYERS, BATCH, D), BF16),
            pltpu.VMEM((2, D, CHUNK), BF16),
            pltpu.VMEM((2, D, CHUNK), BF16),
            pltpu.VMEM((BATCH, CHUNK), F32),
            pltpu.VMEM((CHUNK, D), BF16),
            pltpu.VMEM((BATCH, CHUNK), BF16),
            pltpu.VMEM((WAYS, ROWS, D), F32),
            pltpu.VMEM((4, ROWS, D), F32),
            pltpu.VMEM((2, ROWS, D // 2), F32),
            pltpu.VMEM((2, ROWS, D // 2), F32),
            pltpu.VMEM((ROWS, D // 2), F32),
            pltpu.VMEM((ROWS, D // 2), F32),
            pltpu.VMEM((LAYERS, ROWS, SLAB, HEAD), BF16),
            pltpu.VMEM((LAYERS, ROWS, SLAB, HEAD), BF16),
            pltpu.VMEM((D, CHUNK), BF16),
            dma((WAYS,)), dma((WAYS,)),
            dma((LAYERS, 4, 2)), dma((LAYERS, 4, 2)),
            dma((LAYERS, 4, 4)), dma((LAYERS, 4, 4)),
            dma((LAYERS * CHUNKS, 2)), dma((LAYERS * CHUNKS, 2)),
            dma((LAYERS, WAYS)), dma((LAYERS, WAYS)),
            dma((3, len(PIECES), 4)), dma((3, len(PIECES), 4)),
            dma((2,)), dma((2, 2)), dma((2, 2)), dma((2,)), dma((LAYERS, 4)),
        ],
        compiler_params=pltpu.CompilerParams(collective_id=0, has_side_effects=True, vmem_limit_bytes=63 * 2**20),
        cost_estimate=pl.CostEstimate(flops=60 * 10**9, bytes_accessed=300 * 10**6, transcendentals=0),
    )(*operands)


COPY_ROWS = 16


def slab_base(positions, s):
    return pl.multiple_of((positions[s] // SLAB) * SLAB, SLAB)


def copy_kernel(positions, k_in, v_in, k_out, v_out, k_slabs, v_slabs):
    k_out[...] = k_in[...]
    v_out[...] = v_in[...]
    first = pl.program_id(1) * COPY_ROWS
    for j in range(COPY_ROWS):
        base = slab_base(positions, first + j)
        k_slabs[0, j] = k_in[0, j, pl.ds(base, SLAB), :]
        v_slabs[0, j] = v_in[0, j, pl.ds(base, SLAB), :]


def copy_caches(positions, k_cache, v_cache):
    spec = pl.BlockSpec((1, COPY_ROWS, SMAX, HEAD), lambda l, i: (l, i, 0, 0))
    slab_spec = pl.BlockSpec((1, COPY_ROWS, SLAB, HEAD), lambda l, i: (l, i, 0, 0))
    shape = jax.ShapeDtypeStruct(k_cache.shape, k_cache.dtype)
    slab_shape = jax.ShapeDtypeStruct((LAYERS, ROWS, SLAB, HEAD), k_cache.dtype)
    return pl.pallas_call(
        copy_kernel, name="copy_caches", grid=(LAYERS, ROWS // COPY_ROWS),
        in_specs=[pl.BlockSpec(memory_space=pltpu.SMEM), spec, spec], out_specs=[spec, spec, slab_spec, slab_spec],
        out_shape=[shape, shape, slab_shape, slab_shape],
        compiler_params=pltpu.CompilerParams(vmem_limit_bytes=40 * 2**20),
        cost_estimate=pl.CostEstimate(flops=20 * 10**9, bytes_accessed=4 * k_cache.size * 2, transcendentals=0),
    )(positions, k_cache, v_cache)


def place_kernel(positions, k_slabs, v_slabs, k_in, v_in, k_out, v_out, k_slab, v_slab, sems):
    def place(ref, l, s):
        return ref.at[l, s, pl.ds(slab_base(positions, s), SLAB), :]

    ins = [pltpu.make_async_copy(src.at[l], dst.at[l], sems.at[0, 2 * l + i])
           for l in range(LAYERS) for i, (src, dst) in enumerate(((k_slabs, k_slab), (v_slabs, v_slab)))]
    for c in ins:
        c.start()
    for l in range(LAYERS):
        ins[2 * l].wait()
        ins[2 * l + 1].wait()

        @pl.loop(0, ROWS // 4)
        def _(i, l=l):
            for j in range(4):
                s = i * 4 + j
                pltpu.make_async_copy(k_slab.at[l, s], place(k_out, l, s), sems.at[1, 0]).start()
                pltpu.make_async_copy(v_slab.at[l, s], place(v_out, l, s), sems.at[1, 1]).start()

    pltpu.make_async_copy(k_slab, k_slab, sems.at[1, 0]).wait()
    pltpu.make_async_copy(v_slab, v_slab, sems.at[1, 1]).wait()


def place_rows(positions, k_slabs, v_slabs, k_copy, v_copy):
    any_spec = pl.BlockSpec(memory_space=pl.ANY)
    shape = jax.ShapeDtypeStruct(k_copy.shape, k_copy.dtype)
    slab = pltpu.VMEM((LAYERS, ROWS, SLAB, HEAD), BF16)
    return pl.pallas_call(
        place_kernel, name="place_rows",
        in_specs=[pl.BlockSpec(memory_space=pltpu.SMEM)] + [any_spec] * 4,
        out_specs=[any_spec, any_spec], out_shape=[shape, shape], input_output_aliases={3: 0, 4: 1},
        scratch_shapes=[slab, slab, pltpu.SemaphoreType.DMA((2, 4))],
        compiler_params=pltpu.CompilerParams(vmem_limit_bytes=63 * 2**20),
    )(positions, k_slabs, v_slabs, k_copy, v_copy)


def solution(mesh):
    batch_spec = P(("dp", "w"))
    cache_spec = P(None, ("dp", "w"))
    gain_spec = P(None, "w")
    weight_spec = P(None, "w", None)
    x_swap = [(s, s ^ 2) for s in range(WAYS)]
    y_swap = [(s, s ^ 4) for s in range(WAYS)]

    def per_device(hidden, positions, k_cache, v_cache, attn_norm, w_query, w_key, w_value, w_out, mlp_norm, w_gate, w_up, w_down):
        attn_weights = (w_query, w_key, w_value, w_out)
        from_x = tuple(lax.ppermute(w, "w", x_swap) for w in attn_weights)
        from_y = tuple(lax.ppermute(w, "w", y_swap) for w in attn_weights)
        cos_tab, sin_tab = rope_tables(positions)
        pos_rep = jnp.repeat(positions, HEADS)[:, None]
        gains = jnp.concatenate([attn_norm, mlp_norm, attn_norm, mlp_norm], axis=0)
        k_in, v_in, cos_tab, sin_tab, pos_rep, gains = lax.optimization_barrier((k_cache[:, :, 0], v_cache[:, :, 0], cos_tab, sin_tab, pos_rep, gains))
        k_copy, v_copy, k_slabs, v_slabs = copy_caches(positions, k_in, v_in)
        outs = run_layers(hidden, pos_rep, cos_tab, sin_tab, gains, k_copy, v_copy, k_slabs, v_slabs, *attn_weights, *from_x, *from_y, w_gate, w_up, w_down)
        k_out, v_out = place_rows(positions, outs[1], outs[2], k_copy, v_copy)
        return outs[0], k_out[:, :, None], v_out[:, :, None]

    in_specs = (batch_spec, batch_spec, cache_spec, cache_spec, gain_spec, weight_spec, weight_spec, weight_spec, weight_spec, gain_spec, weight_spec, weight_spec, weight_spec)
    out_specs = (batch_spec, cache_spec, cache_spec)
    return jax.shard_map(per_device, mesh=mesh, in_specs=in_specs, out_specs=out_specs, check_vma=False)
```

```python
import jax
import jax.numpy as jnp
from jax import lax
from jax.experimental import pallas as pl
from jax.experimental.pallas import tpu as pltpu
from jax.sharding import PartitionSpec as P

EPS = 1e-6
ROPE_BASE = 10000.0
MESH = pl.DeviceIdType.MESH
BF16 = jnp.bfloat16
F32 = jnp.float32

WAYS = 8
LAYERS = 2
ROWS = 128
BATCH = ROWS * WAYS
D = 2048
SHARD = D // WAYS
HEADS = 8
HEAD = 256
HALF = HEAD // 2
SMAX = 256
FF_BLOCK = 2048
CHUNK = 256
CHUNKS = FF_BLOCK // CHUNK
GROUP = 8
GROUPS = ROWS // GROUP
SUB = 512
PIECES = ((0, 256), (1024, 256), (256, 512), (1280, 512), (768, 256), (1792, 256))
SLAB = 16
PEERS = (6, 7, 2, 4, 3, 5, 1)
AHEAD = 2
MROWS = 512
DROWS = 512


def rope_tables(positions):
    inv_freq = ROPE_BASE ** (-2.0 * jnp.arange(HALF, dtype=F32) / HEAD)
    angles = positions.astype(F32)[:, None] * inv_freq[None, :]
    return jnp.cos(angles), jnp.sin(angles)


def al(index, size):
    return pl.ds(pl.multiple_of(index * size, size), size)


def layers_kernel(hid_in, pos_in, cos_in, sin_in, gains_own, k_cache, v_cache, k_slabs, v_slabs,
                  wq, wk, wv, wo, qx, kx, vx, ox, qy, ky, vy, oy, w_gate, w_up, w_down,
                  hid_out, k_slabs_out, v_slabs_out, qbuf, kbuf, vbuf, obuf, gbuf, ubuf,
                  gains_all, hid, x_act, q_head, q_seq, a_seq, a_flat, kn, vn, kv_k, kv_v, w_tile,
                  y_full, g_tile, u_tile, gate_act, d_tile, m_act, acc, core_recv, p1a, p1b, p2a, p2b, k_slab, v_slab, u_last, pos_rep, cos_ref, sin_ref,
                  gain_s, gain_r, fwd_s, fwd_r, rel_s, rel_r, chunk_s, chunk_r, y_s, y_r,
                  rs_s, rs_r, tile_sem, kv_sem, gate_sem, down_sem, slab_sem, load_sem, store_sem):
    me = lax.axis_index("w")
    core = lax.rem(me, 2)
    xbit = lax.rem(me // 2, 2)
    ybit = me // 4
    peer = [jnp.bitwise_xor(me, m) for m in range(WAYS)]

    def send(src, dst, m, ssem, rsem):
        return pltpu.make_async_remote_copy(src_ref=src, dst_ref=dst, send_sem=ssem, recv_sem=rsem,
                                            device_id={"w": peer[m]}, device_id_type=MESH)

    loads = [pltpu.make_async_copy(src, dst, load_sem.at[i]) for i, (src, dst) in enumerate((
        (gains_own, gains_all.at[me]), (hid_in, hid), (cos_in, cos_ref), (sin_in, sin_ref), (pos_in, pos_rep)))]
    for c in loads:
        c.start()

    barrier = pltpu.get_barrier_semaphore()
    for m in range(1, WAYS):
        pl.semaphore_signal(barrier, inc=1, device_id={"w": peer[m]}, device_id_type=MESH)
    pl.semaphore_wait(barrier, WAYS - 1)

    own = (wq, wk, wv, wo)
    from_x = (qx, kx, vx, ox)
    from_y = (qy, ky, vy, oy)
    bufs = (qbuf, kbuf, vbuf, obuf)
    half = SHARD // 2

    def forwards(l, a):
        return (send(from_x[a].at[l, pl.ds(0, half)], bufs[a].at[l, 6, pl.ds(0, half)], 4, fwd_s.at[l, a], fwd_r.at[l, a]),
                send(from_y[a].at[l, pl.ds(half, half)], bufs[a].at[l, 6, pl.ds(half, half)], 2, fwd_s.at[l, a], fwd_r.at[l, a]))

    def relay(l, a, i):
        src = (own[a], from_x[a], from_y[a])[i].at[l] if i < 3 else bufs[a].at[l, 6]
        return send(src, bufs[a].at[l, 2 * i + 1], 1, rel_s.at[l, a], rel_r.at[l, a])

    def forwards_wait(sems, l, a):
        pltpu.make_async_copy(bufs[a].at[l, 6], bufs[a].at[l, 6], sems.at[l, a]).wait()

    def relays_wait(sems, l, a):
        part = bufs[a].at[l, pl.ds(0, 4)]
        pltpu.make_async_copy(part, part, sems.at[l, a]).wait()

    def weights_start(l):
        for a in range(4):
            for c in forwards(l, a):
                c.start()
        for a in range(4):
            for i in range(3):
                relay(l, a, i).start()

    def weights_relay_last(l, a):
        forwards_wait(fwd_r, l, a)
        relay(l, a, 3).start()

    def weights_arrived(l, a):
        relays_wait(rel_r, l, a)

    ffw = (w_gate, w_up)
    ffbuf = (gbuf, ubuf)

    def unit_start(g, s):
        l, k = g // CHUNKS, lax.rem(g, CHUNKS)
        for m in PEERS:
            cols = pl.ds(pl.multiple_of(peer[m] * FF_BLOCK + k * CHUNK, CHUNK), CHUNK)
            send(ffw[s].at[l, :, cols], ffbuf[s].at[l, k, al(me, SHARD)], m, chunk_s.at[g, s], chunk_r.at[g, s]).start()

    last_g = LAYERS * CHUNKS - 1
    last_own = pltpu.make_async_copy(
        w_up.at[LAYERS - 1, :, pl.ds(pl.multiple_of(me * FF_BLOCK + (CHUNKS - 1) * CHUNK, CHUNK), CHUNK)], u_last.at[al(me, SHARD)], down_sem.at[1])
    last_own.start()

    def last_up_start():
        for m in PEERS:
            cols = pl.ds(pl.multiple_of(peer[m] * FF_BLOCK + (CHUNKS - 1) * CHUNK, CHUNK), CHUNK)
            send(w_up.at[LAYERS - 1, :, cols], u_last.at[al(me, SHARD)], m, chunk_s.at[last_g, 1], chunk_r.at[last_g, 1]).start()

    def last_up_wait():
        last_own.wait()
        part = u_last.at[pl.ds(0, (WAYS - 1) * SHARD)]
        pltpu.make_async_copy(part, part, chunk_r.at[last_g, 1]).wait()

    def unit_wait(sem, g, s):
        l, k = g // CHUNKS, lax.rem(g, CHUNKS)
        part = ffbuf[s].at[l, k, pl.ds(0, (WAYS - 1) * SHARD)]
        pltpu.make_async_copy(part, part, sem.at[g, s]).wait()

    weights_start(0)

    gain_copies = [send(gains_own, gains_all.at[me], m, gain_s.at[m], gain_r.at[m]) for m in range(1, WAYS)]
    for c in gain_copies:
        c.start()

    @pl.loop(0, AHEAD)
    def _(g):
        unit_start(g, 0)
        unit_start(g, 1)

    for c in gain_copies:
        c.wait_recv()

    def norm_into(src, gain_row, dst, dst_row0):
        @pl.loop(0, ROWS // 32)
        def _(i):
            h = src[al(i, 32), :].astype(F32)
            r = lax.rsqrt(jnp.mean(h * h, axis=-1, keepdims=True) + EPS)
            for s in range(WAYS):
                cols = pl.ds(s * SHARD, SHARD)
                g = 1.0 + gains_all[s, pl.ds(gain_row, 1), :]
                dst[pl.ds(pl.multiple_of(dst_row0 + i * 32, 32), 32), cols] = (h[:, s * SHARD:(s + 1) * SHARD] * r * g).astype(BF16)

    def tile_copies(l, a, n, slot):
        cols = al(n, HEAD)
        srcs = (own[a].at[l], bufs[a].at[l, 1], from_x[a].at[l], bufs[a].at[l, 3],
                from_y[a].at[l], bufs[a].at[l, 5], bufs[a].at[l, 6], bufs[a].at[l, 7])
        return [pltpu.make_async_copy(srcs[m].at[:, cols], w_tile.at[slot, al(peer[m], SHARD)], tile_sem.at[slot])
                for m in range(WAYS)]

    def tile_start(l, a, n, slot):
        for c in tile_copies(l, a, n, slot):
            c.start()

    def tile_wait(slot):
        pltpu.make_async_copy(w_tile.at[slot], w_tile.at[slot], tile_sem.at[slot]).wait()

    def rope(vec):
        lead, tail = vec[:, :HALF], vec[:, HALF:]
        cos_b, sin_b = cos_ref[...], sin_ref[...]
        return jnp.concatenate([lead * cos_b - tail * sin_b, tail * cos_b + lead * sin_b], axis=-1)

    def kv_copies(l, i, slot):
        return (pltpu.make_async_copy(k_cache.at[l, al(i, GROUP)], kv_k.at[slot], kv_sem.at[slot, 0]),
                pltpu.make_async_copy(v_cache.at[l, al(i, GROUP)], kv_v.at[slot], kv_sem.at[slot, 1]))

    def kv_start(l, i, slot):
        for c in kv_copies(l, i, slot):
            c.start()

    def attention_step(l, i):
        slot = lax.rem(i, 2)

        @pl.when(i + 1 < GROUPS)
        def _():
            kv_start(l, i + 1, 1 - slot)

        for c in kv_copies(l, i, slot):
            c.wait()
        rows = GROUP * HEADS
        q64 = q_seq[al(i, GROUP)].reshape(rows, HEAD)
        kn64 = jnp.broadcast_to(kn[al(i, GROUP), :][:, None, :], (GROUP, HEADS, HEAD)).reshape(rows, HEAD)
        vn64 = jnp.broadcast_to(vn[al(i, GROUP), :][:, None, :], (GROUP, HEADS, HEAD)).reshape(rows, HEAD)
        pos = pos_rep[al(i, rows), :]
        scores = jnp.concatenate(
            [lax.dot_general(q64[s * HEADS:(s + 1) * HEADS].astype(BF16), kv_k[slot, s], (((1,), (1,)), ((), ())), preferred_element_type=F32)
             for s in range(GROUP)], axis=0)
        new_score = jnp.sum(q64 * kn64, axis=-1, keepdims=True)
        place = lax.broadcasted_iota(jnp.int32, (rows, SMAX), 1)
        is_new = place == pos
        scores = jnp.where(is_new, new_score, scores)
        scores = jnp.where(place <= pos, scores, -1e30)
        u = jnp.exp(scores - jnp.max(scores, axis=-1, keepdims=True))
        den = jnp.sum(u, axis=-1, keepdims=True)
        u_new = jnp.sum(jnp.where(is_new, u, 0.0), axis=-1, keepdims=True).astype(BF16).astype(F32)
        u_old = jnp.where(is_new, 0.0, u)
        vals = jnp.concatenate(
            [jnp.dot(u_old[s * HEADS:(s + 1) * HEADS].astype(BF16), kv_v[slot, s], preferred_element_type=F32)
             for s in range(GROUP)], axis=0)
        vals = (vals + u_new * vn64) / den
        a_seq[al(i, GROUP)] = vals.reshape(GROUP, HEADS, HEAD)

    def y_send(l, m):
        mine = y_full.at[l, al(me, ROWS)]
        return send(mine, mine, m, y_s.at[l, m], y_r.at[l, m])

    def y_forward(l, m):
        first = 0 if m == 2 else ROWS // 2
        block = y_full.at[l, pl.ds(pl.multiple_of(peer[m] * ROWS + first, ROWS // 2), ROWS // 2)]
        i = 6 if m == 2 else 0
        return send(block, block, 6 - m, y_s.at[l, i], y_r.at[l, i])

    def y_relay(l, m):
        block = y_full.at[l, al(peer[m], ROWS)]
        return send(block, block, 1, y_s.at[l, m + 1], y_r.at[l, m + 1])

    fftile = (g_tile, u_tile)

    def tile_in(l, k, s):
        unit_wait(chunk_r, l * CHUNKS + k, s)
        slot = lax.rem(k, 2)
        own_cols = pl.ds(pl.multiple_of(me * FF_BLOCK + k * CHUNK, CHUNK), CHUNK)
        for m in range(WAYS):
            src = ffw[s].at[l, :, own_cols] if m == 0 else ffbuf[s].at[l, k, al(peer[m], SHARD)]
            pltpu.make_async_copy(src, fftile[s].at[slot, al(peer[m], SHARD)], gate_sem.at[s, slot]).start()

    def tile_ready(k, s):
        slot = lax.rem(k, 2)
        pltpu.make_async_copy(fftile[s].at[slot], fftile[s].at[slot], gate_sem.at[s, slot]).wait()

    def mlp_chunk(l, k, last, down):
        slot = lax.rem(k, 2)
        d_copy = pltpu.make_async_copy(w_down.at[l, al(k, CHUNK)], d_tile, down_sem.at[0])
        d_copy.start()
        tile_ready(k, 0)
        if not last:
            tile_in(l, k, 1)

        @pl.loop(0, BATCH // MROWS)
        def _(i):
            gate = jnp.dot(y_full[l, al(i, MROWS), :], g_tile[slot], preferred_element_type=F32)
            gate_act[al(i, MROWS), :] = jax.nn.gelu(gate, approximate=True)

        direct = last and l == LAYERS - 1
        if direct:
            last_up_wait()
        else:
            if last:
                tile_in(l, k, 1)
            tile_ready(k, 1)

        @pl.loop(0, BATCH // MROWS)
        def _(i):
            u_cols = u_last[...] if direct else u_tile[slot]
            up = jnp.dot(y_full[l, al(i, MROWS), :], u_cols, preferred_element_type=F32)
            m_act[al(i, MROWS), :] = (gate_act[al(i, MROWS), :] * up).astype(BF16)

        if not last:
            tile_in(l, k + 1, 0)
        d_copy.wait()
        down()

    def down_piece(cols, first):
        @pl.loop(0, BATCH // DROWS)
        def _(i):
            part = jnp.dot(m_act[al(i, DROWS), :], d_tile[:, cols], preferred_element_type=F32)
            for b in range(DROWS // ROWS):
                blk = i * (DROWS // ROWS) + b
                piece = part[b * ROWS:(b + 1) * ROWS]
                acc[blk, :, cols] = piece if first else acc[blk, :, cols] + piece

    half_d = D // 2

    def piece(s):
        start, width = PIECES[s]
        return start < half_d, pl.ds(start, width), pl.ds(start % half_d, width)

    def rs_core(s):
        _, cols, _ = piece(s)
        return [send(acc.at[2 * j + 1 - core, :, cols], core_recv.at[j, :, cols], 1, rs_s.at[0, s], rs_r.at[0, s]) for j in range(4)]

    def rs_first(s):
        left, cols, local = piece(s)
        if left:
            return [send(acc.at[2 * (2 * t + 1 - xbit) + core, :, cols], p1a.at[t, :, local], 2, rs_s.at[1, s], rs_r.at[1, s]) for t in range(2)]
        return [send(acc.at[2 * (2 * (1 - ybit) + t) + core, :, cols], p1b.at[t, :, local], 4, rs_s.at[1, s], rs_r.at[1, s]) for t in range(2)]

    def rs_second(s):
        left, cols, local = piece(s)
        if left:
            return [send(acc.at[2 * (2 * (1 - ybit) + xbit) + core, :, cols], p2a.at[:, local], 4, rs_s.at[2, s], rs_r.at[2, s])]
        return [send(acc.at[2 * (2 * ybit + 1 - xbit) + core, :, cols], p2b.at[:, local], 2, rs_s.at[2, s], rs_r.at[2, s])]

    def rs_wait(sems, phase, s):
        left, cols, local = piece(s)
        ref = (core_recv.at[:, :, cols], (p1a if left else p1b).at[:, :, local], (p2a if left else p2b).at[:, local])[phase]
        pltpu.make_async_copy(ref, ref, sems.at[phase, s]).wait()

    def rs_core_add(s):
        _, cols, _ = piece(s)
        rs_wait(rs_r, 0, s)

        @pl.loop(0, 4)
        def _(j):
            acc[2 * j + core, :, cols] = acc[2 * j + core, :, cols] + core_recv[j, :, cols]

    def rs_first_add(s):
        left, cols, local = piece(s)
        rs_wait(rs_r, 1, s)

        @pl.loop(0, 2)
        def _(t):
            if left:
                blk = 2 * (2 * t + xbit) + core
                acc[blk, :, cols] = acc[blk, :, cols] + p1a[t, :, local]
            else:
                blk = 2 * (2 * ybit + t) + core
                acc[blk, :, cols] = acc[blk, :, cols] + p1b[t, :, local]

    def rs_second_add(s):
        left, cols, local = piece(s)
        rs_wait(rs_r, 2, s)
        other = p2a[:, local] if left else p2b[:, local]
        total = acc[me, :, cols] + other
        hid[:, cols] = (hid[:, cols].astype(F32) + total).astype(BF16)

    def slab_in(l):
        return (pltpu.make_async_copy(k_slabs.at[l], k_slab.at[l], slab_sem.at[l, 0]),
                pltpu.make_async_copy(v_slabs.at[l], v_slab.at[l], slab_sem.at[l, 1]))

    def slab_out(l):
        return (pltpu.make_async_copy(k_slab.at[l], k_slabs_out.at[l], slab_sem.at[l, 2]),
                pltpu.make_async_copy(v_slab.at[l], v_slabs_out.at[l], slab_sem.at[l, 3]))

    def slab_fill(l):
        for c in slab_in(l):
            c.wait()
        row = lax.broadcasted_iota(jnp.int32, (SLAB, HEAD), 0)

        @pl.loop(0, GROUPS)
        def _(i):
            k8 = kn[al(i, GROUP), :]
            v8 = vn[al(i, GROUP), :]
            pos = pos_rep[al(i, GROUP * HEADS), :]
            for j in range(GROUP):
                q = i * GROUP + j
                hit = row == jnp.bitwise_and(pos[j * HEADS:j * HEADS + 1], SLAB - 1)
                k_slab[l, q] = jnp.where(hit, k8[j:j + 1], k_slab[l, q].astype(F32)).astype(BF16)
                v_slab[l, q] = jnp.where(hit, v8[j:j + 1], v_slab[l, q].astype(F32)).astype(BF16)

        for c in slab_out(l):
            c.start()

    order = range(len(PIECES))

    def hid_store(s):
        cols = pl.ds(*PIECES[s])
        return pltpu.make_async_copy(hid.at[:, cols], hid_out.at[:, cols], store_sem.at[s])

    def sends_over():
        for c in gain_copies:
            c.wait_send()
        for l in range(LAYERS):
            for a in range(4):
                forwards_wait(fwd_s, l, a)
                relays_wait(rel_s, l, a)
            for m in (2, 4, 1):
                y_send(l, m).wait_send()
            for m in (2, 4):
                y_forward(l, m).wait_send()
            for m in (2, 4, 6):
                y_relay(l, m).wait_send()

        @pl.loop(0, LAYERS * CHUNKS)
        def _(g):
            unit_wait(chunk_s, g, 0)
            unit_wait(chunk_s, g, 1)

        for l in range(LAYERS):
            for c in slab_out(l):
                c.wait()

    for l in range(LAYERS):
        for c in slab_in(l):
            c.start()

    for c in loads:
        c.wait()

    for l in range(LAYERS):
        base = l * CHUNKS
        norm_into(hid, l, x_act, 0)
        if l == 0:
            for a in range(3):
                weights_relay_last(l, a)
        kv_start(l, 0, 0)
        for a in range(3):
            weights_arrived(l, a)
        tile_start(l, 0, 0, 0)

        @pl.loop(0, HEADS)
        def _(h, l=l):
            slot = lax.rem(h, 2)

            @pl.when(h + 1 < HEADS)
            def _():
                tile_start(l, 0, h + 1, 1 - slot)

            tile_wait(slot)
            q = rope(jnp.dot(x_act[...], w_tile[slot], preferred_element_type=F32))
            q_head[h] = (q * HEAD ** -0.5).astype(BF16).astype(F32)

        tile_start(l, 1, 0, 0)
        tile_start(l, 2, 0, 1)
        for h in range(HEADS):
            q_seq[:, h, :] = q_head[h]
        tile_wait(0)
        kn[...] = rope(jnp.dot(x_act[...], w_tile[0], preferred_element_type=F32)).astype(BF16).astype(F32)
        tile_wait(1)
        vn[...] = jnp.dot(x_act[...], w_tile[1], preferred_element_type=F32).astype(BF16).astype(F32)

        if l == 0:
            weights_relay_last(l, 3)
        else:
            unit_start(base + 2, 0)

        @pl.loop(0, GROUPS // 2)
        def _(i, l=l):
            attention_step(l, i)

        unit_start(base + 2, l)

        @pl.loop(GROUPS // 2, GROUPS)
        def _(i, l=l):
            attention_step(l, i)

        if l == 0:
            unit_start(base + 2, 1)
        for h in range(HEADS):
            a_flat[:, pl.ds(h * HEAD, HEAD)] = a_seq[:, h, :].astype(BF16)
        weights_arrived(l, 3)
        tile_start(l, 3, 0, 0)

        @pl.loop(0, HEADS)
        def _(n, l=l):
            slot = lax.rem(n, 2)

            @pl.when(n + 1 < HEADS)
            def _():
                tile_start(l, 3, n + 1, 1 - slot)

            tile_wait(slot)
            cols = al(n, HEAD)
            part = jnp.dot(a_flat[...], w_tile[slot], preferred_element_type=F32)
            hid[:, cols] = (hid[:, cols].astype(F32) + part).astype(BF16)

        norm_into(hid, LAYERS + l, y_full.at[l], me * ROWS)
        for m in (2, 4, 1):
            y_send(l, m).start()
        unit_start(base + 3, 0)
        for m in (2, 4):
            y_send(l, m).wait_recv()
            y_forward(l, m).start()
        unit_start(base + 3, 1)
        for m in (2, 4):
            y_relay(l, m).start()
        for m in (2, 4):
            y_forward(l, m).wait_recv()
        y_relay(l, 6).start()
        y_send(l, 1).wait_recv()
        for m in (2, 4, 6):
            y_relay(l, m).wait_recv()

        if l == 0:
            weights_start(1)

        @pl.loop(base + 4, base + CHUNKS - l)
        def _(g):
            unit_start(g, 0)
            unit_start(g, 1)

        if l == LAYERS - 1:
            unit_start(last_g, 0)
            last_up_start()

        def first_down():
            @pl.loop(0, D // SUB)
            def _(s):
                down_piece(al(s, SUB), True)

        def more_down():
            @pl.loop(0, D // SUB)
            def _(s):
                down_piece(al(s, SUB), False)

        tile_in(l, 0, 0)
        mlp_chunk(l, 0, False, first_down)

        @pl.loop(1, CHUNKS - 1)
        def _(k, l=l):
            mlp_chunk(l, k, False, more_down)

        if l == 0:
            for a in range(4):
                weights_relay_last(1, a)
            unit_start(CHUNKS, 0)

        def last_down():
            for s in order:
                down_piece(pl.ds(*PIECES[s]), False)
                for c in rs_core(s):
                    c.start()

        mlp_chunk(l, CHUNKS - 1, True, last_down)
        for s in order:
            rs_core_add(s)
            for c in rs_first(s):
                c.start()
        if l == 0:
            unit_start(CHUNKS, 1)
        slab_fill(l)
        if l == LAYERS - 1:
            sends_over()
        for s in order:
            rs_first_add(s)
            for c in rs_second(s):
                c.start()
        if l == 0:
            unit_start(CHUNKS + 1, 0)
            unit_start(CHUNKS + 1, 1)
        for s in order:
            rs_second_add(s)
            if l == LAYERS - 1:
                hid_store(s).start()
        if l == 0:
            for s in order:
                for phase in range(3):
                    rs_wait(rs_s, phase, s)

    for s in order:
        hid_store(s).wait()
        for phase in range(3):
            rs_wait(rs_s, phase, s)


def run_layers(*operands):
    any_spec = pl.BlockSpec(memory_space=pl.ANY)
    sds = jax.ShapeDtypeStruct
    dma = pltpu.SemaphoreType.DMA
    return pl.pallas_call(
        layers_kernel,
        name="layers",
        out_shape=[
            sds((ROWS, D), BF16), sds((LAYERS, ROWS, SLAB, HEAD), BF16), sds((LAYERS, ROWS, SLAB, HEAD), BF16),
            sds((LAYERS, WAYS, SHARD, D), BF16), sds((LAYERS, WAYS, SHARD, HEAD), BF16),
            sds((LAYERS, WAYS, SHARD, HEAD), BF16), sds((LAYERS, WAYS, SHARD, D), BF16),
            sds((LAYERS, CHUNKS, D, CHUNK), BF16), sds((LAYERS, CHUNKS, D, CHUNK), BF16),
        ],
        in_specs=[any_spec] * 24,
        out_specs=[any_spec] * 9,
        scratch_shapes=[
            pltpu.VMEM((WAYS, 8, SHARD), F32),
            pltpu.VMEM((ROWS, D), BF16),
            pltpu.VMEM((ROWS, D), BF16),
            pltpu.VMEM((HEADS, ROWS, HEAD), F32),
            pltpu.VMEM((ROWS, HEADS, HEAD), F32),
            pltpu.VMEM((ROWS, HEADS, HEAD), F32),
            pltpu.VMEM((ROWS, D), BF16),
            pltpu.VMEM((ROWS, HEAD), F32),
            pltpu.VMEM((ROWS, HEAD), F32),
            pltpu.VMEM((2, GROUP, SMAX, HEAD), BF16),
            pltpu.VMEM((2, GROUP, SMAX, HEAD), BF16),
            pltpu.VMEM((2, D, HEAD), BF16),
            pltpu.VMEM((LAYERS, BATCH, D), BF16),
            pltpu.VMEM((2, D, CHUNK), BF16),
            pltpu.VMEM((2, D, CHUNK), BF16),
            pltpu.VMEM((BATCH, CHUNK), F32),
            pltpu.VMEM((CHUNK, D), BF16),
            pltpu.VMEM((BATCH, CHUNK), BF16),
            pltpu.VMEM((WAYS, ROWS, D), F32),
            pltpu.VMEM((4, ROWS, D), F32),
            pltpu.VMEM((2, ROWS, D // 2), F32),
            pltpu.VMEM((2, ROWS, D // 2), F32),
            pltpu.VMEM((ROWS, D // 2), F32),
            pltpu.VMEM((ROWS, D // 2), F32),
            pltpu.VMEM((LAYERS, ROWS, SLAB, HEAD), BF16),
            pltpu.VMEM((LAYERS, ROWS, SLAB, HEAD), BF16),
            pltpu.VMEM((D, CHUNK), BF16),
            pltpu.VMEM((BATCH, 1), jnp.int32),
            pltpu.VMEM((ROWS, HALF), F32),
            pltpu.VMEM((ROWS, HALF), F32),
            dma((WAYS,)), dma((WAYS,)),
            dma((LAYERS, 4)), dma((LAYERS, 4)),
            dma((LAYERS, 4)), dma((LAYERS, 4)),
            dma((LAYERS * CHUNKS, 2)), dma((LAYERS * CHUNKS, 2)),
            dma((LAYERS, WAYS)), dma((LAYERS, WAYS)),
            dma((3, len(PIECES))), dma((3, len(PIECES))),
            dma((2,)), dma((2, 2)), dma((2, 2)), dma((2,)), dma((LAYERS, 4)), dma((5,)), dma((len(PIECES),)),
        ],
        compiler_params=pltpu.CompilerParams(collective_id=0, has_side_effects=True, vmem_limit_bytes=63 * 2**20),
        cost_estimate=pl.CostEstimate(flops=60 * 10**9, bytes_accessed=300 * 10**6, transcendentals=0),
    )(*operands)


COPY_ROWS = 16


def slab_base(positions, s):
    return pl.multiple_of((positions[s] // SLAB) * SLAB, SLAB)


def copy_kernel(positions, k_in, v_in, k_out, v_out, k_slabs, v_slabs):
    k_out[...] = k_in[...]
    v_out[...] = v_in[...]
    first = pl.program_id(1) * COPY_ROWS
    for j in range(COPY_ROWS):
        base = slab_base(positions, first + j)
        k_slabs[0, j] = k_in[0, j, pl.ds(base, SLAB), :]
        v_slabs[0, j] = v_in[0, j, pl.ds(base, SLAB), :]


def copy_caches(positions, k_cache, v_cache):
    spec = pl.BlockSpec((1, COPY_ROWS, SMAX, HEAD), lambda l, i: (l, i, 0, 0))
    slab_spec = pl.BlockSpec((1, COPY_ROWS, SLAB, HEAD), lambda l, i: (l, i, 0, 0))
    shape = jax.ShapeDtypeStruct(k_cache.shape, k_cache.dtype)
    slab_shape = jax.ShapeDtypeStruct((LAYERS, ROWS, SLAB, HEAD), k_cache.dtype)
    return pl.pallas_call(
        copy_kernel, name="copy_caches", grid=(LAYERS, ROWS // COPY_ROWS),
        in_specs=[pl.BlockSpec(memory_space=pltpu.SMEM), spec, spec], out_specs=[spec, spec, slab_spec, slab_spec],
        out_shape=[shape, shape, slab_shape, slab_shape],
        compiler_params=pltpu.CompilerParams(vmem_limit_bytes=40 * 2**20),
        cost_estimate=pl.CostEstimate(flops=20 * 10**9, bytes_accessed=4 * k_cache.size * 2, transcendentals=0),
    )(positions, k_cache, v_cache)


def place_kernel(positions, hid_in, k_slabs, v_slabs, k_in, v_in, hid_out, k_out, v_out, hid, k_slab, v_slab, sems):
    def place(ref, l, s):
        return ref.at[l, s, pl.ds(slab_base(positions, s), SLAB), :]

    ins = [pltpu.make_async_copy(src.at[l], dst.at[l], sems.at[0, 2 * l + i])
           for l in range(LAYERS) for i, (src, dst) in enumerate(((k_slabs, k_slab), (v_slabs, v_slab)))]
    for c in ins:
        c.start()
    hid_load = pltpu.make_async_copy(hid_in, hid, sems.at[1, 2])
    hid_load.start()
    for l in range(LAYERS):
        ins[2 * l].wait()
        ins[2 * l + 1].wait()

        @pl.loop(0, ROWS // 4)
        def _(i, l=l):
            for j in range(4):
                s = i * 4 + j
                pltpu.make_async_copy(k_slab.at[l, s], place(k_out, l, s), sems.at[1, 0]).start()
                pltpu.make_async_copy(v_slab.at[l, s], place(v_out, l, s), sems.at[1, 1]).start()

    hid_load.wait()
    hid_store = pltpu.make_async_copy(hid, hid_out, sems.at[1, 3])
    hid_store.start()
    pltpu.make_async_copy(k_slab, k_slab, sems.at[1, 0]).wait()
    pltpu.make_async_copy(v_slab, v_slab, sems.at[1, 1]).wait()
    hid_store.wait()


def place_rows(positions, hidden, k_slabs, v_slabs, k_copy, v_copy):
    any_spec = pl.BlockSpec(memory_space=pl.ANY)
    shape = jax.ShapeDtypeStruct(k_copy.shape, k_copy.dtype)
    slab = pltpu.VMEM((LAYERS, ROWS, SLAB, HEAD), BF16)
    return pl.pallas_call(
        place_kernel, name="place_rows",
        in_specs=[pl.BlockSpec(memory_space=pltpu.SMEM)] + [any_spec] * 5,
        out_specs=[any_spec] * 3, out_shape=[jax.ShapeDtypeStruct(hidden.shape, hidden.dtype), shape, shape], input_output_aliases={4: 1, 5: 2},
        scratch_shapes=[pltpu.VMEM((ROWS, D), BF16), slab, slab, pltpu.SemaphoreType.DMA((2, 4))],
        compiler_params=pltpu.CompilerParams(vmem_limit_bytes=63 * 2**20),
    )(positions, hidden, k_slabs, v_slabs, k_copy, v_copy)


def solution(mesh):
    batch_spec = P(("dp", "w"))
    cache_spec = P(None, ("dp", "w"))
    gain_spec = P(None, "w")
    weight_spec = P(None, "w", None)
    x_swap = [(s, s ^ 2) for s in range(WAYS)]
    y_swap = [(s, s ^ 4) for s in range(WAYS)]

    def per_device(hidden, positions, k_cache, v_cache, attn_norm, w_query, w_key, w_value, w_out, mlp_norm, w_gate, w_up, w_down):
        attn_weights = (w_query, w_key, w_value, w_out)
        from_x = tuple(lax.ppermute(w, "w", x_swap) for w in attn_weights)
        from_y = tuple(lax.ppermute(w, "w", y_swap) for w in attn_weights)
        cos_tab, sin_tab = rope_tables(positions)
        pos_rep = jnp.repeat(positions, HEADS)[:, None]
        gains = jnp.concatenate([attn_norm, mlp_norm, attn_norm, mlp_norm], axis=0)
        k_in, v_in, cos_tab, sin_tab, pos_rep, gains = lax.optimization_barrier((k_cache[:, :, 0], v_cache[:, :, 0], cos_tab, sin_tab, pos_rep, gains))
        k_copy, v_copy, k_slabs, v_slabs = copy_caches(positions, k_in, v_in)
        outs = run_layers(hidden, pos_rep, cos_tab, sin_tab, gains, k_copy, v_copy, k_slabs, v_slabs, *attn_weights, *from_x, *from_y, w_gate, w_up, w_down)
        hidden_out, k_out, v_out = place_rows(positions, outs[0], outs[1], outs[2], k_copy, v_copy)
        return hidden_out, k_out[:, :, None], v_out[:, :, None]

    in_specs = (batch_spec, batch_spec, cache_spec, cache_spec, gain_spec, weight_spec, weight_spec, weight_spec, weight_spec, gain_spec, weight_spec, weight_spec, weight_spec)
    out_specs = (batch_spec, cache_spec, cache_spec)
    return jax.shard_map(per_device, mesh=mesh, in_specs=in_specs, out_specs=out_specs, check_vma=False)
```

```python
import jax
import jax.numpy as jnp
from jax import lax
from jax.experimental import pallas as pl
from jax.experimental.pallas import tpu as pltpu
from jax.sharding import PartitionSpec as P

EPS = 1e-6
ROPE_BASE = 10000.0
MESH = pl.DeviceIdType.MESH
BF16 = jnp.bfloat16
F32 = jnp.float32

WAYS = 8
LAYERS = 2
ROWS = 128
BATCH = ROWS * WAYS
D = 2048
SHARD = D // WAYS
HEADS = 8
HEAD = 256
HALF = HEAD // 2
SMAX = 256
FF_BLOCK = 2048
CHUNK = 256
CHUNKS = FF_BLOCK // CHUNK
GROUP = 8
GROUPS = ROWS // GROUP
SUB = 512
PIECES = ((0, 256), (1024, 256), (256, 512), (1280, 512), (768, 256), (1792, 256))
SLAB = 16
PEERS = (6, 7, 2, 4, 3, 5, 1)
AHEAD = 2
MROWS = 512
DROWS = 512


def rope_tables(positions):
    inv_freq = ROPE_BASE ** (-2.0 * jnp.arange(HALF, dtype=F32) / HEAD)
    angles = positions.astype(F32)[:, None] * inv_freq[None, :]
    return jnp.cos(angles), jnp.sin(angles)


def al(index, size):
    return pl.ds(pl.multiple_of(index * size, size), size)


def layers_kernel(hid_in, pos_in, cos_in, sin_in, gains_own, k_cache, v_cache, k_slabs, v_slabs,
                  wq, wk, wv, wo, qx, kx, vx, ox, qy, ky, vy, oy, w_gate, w_up, w_down,
                  hid_out, k_slabs_out, v_slabs_out, qbuf, kbuf, vbuf, obuf, gbuf, ubuf,
                  gains_all, hid, x_act, q_head, q_seq, a_seq, a_flat, kn, vn, kv_k, kv_v, w_tile,
                  y_full, g_tile, u_tile, gate_act, d_tile, m_act, acc, core_recv, p1a, p1b, p2a, p2b, k_slab, v_slab, u_last, pos_rep, cos_ref, sin_ref,
                  gain_s, gain_r, fwd_s, fwd_r, rel_s, rel_r, chunk_s, chunk_r, y_s, y_r,
                  rs_s, rs_r, tile_sem, kv_sem, gate_sem, down_sem, slab_sem, load_sem, store_sem):
    me = lax.axis_index("w")
    core = lax.rem(me, 2)
    xbit = lax.rem(me // 2, 2)
    ybit = me // 4
    peer = [jnp.bitwise_xor(me, m) for m in range(WAYS)]

    def send(src, dst, m, ssem, rsem):
        return pltpu.make_async_remote_copy(src_ref=src, dst_ref=dst, send_sem=ssem, recv_sem=rsem,
                                            device_id={"w": peer[m]}, device_id_type=MESH)

    loads = [pltpu.make_async_copy(src, dst, load_sem.at[i]) for i, (src, dst) in enumerate((
        (gains_own, gains_all.at[me]), (hid_in, hid), (cos_in, cos_ref), (sin_in, sin_ref), (pos_in, pos_rep)))]
    for c in loads:
        c.start()

    barrier = pltpu.get_barrier_semaphore()
    for m in range(1, WAYS):
        pl.semaphore_signal(barrier, inc=1, device_id={"w": peer[m]}, device_id_type=MESH)
    pl.semaphore_wait(barrier, WAYS - 1)

    own = (wq, wk, wv, wo)
    from_x = (qx, kx, vx, ox)
    from_y = (qy, ky, vy, oy)
    bufs = (qbuf, kbuf, vbuf, obuf)
    half = SHARD // 2

    def forwards(l, a):
        return (send(from_x[a].at[l, pl.ds(0, half)], bufs[a].at[l, 6, pl.ds(0, half)], 4, fwd_s.at[l, a], fwd_r.at[l, a]),
                send(from_y[a].at[l, pl.ds(half, half)], bufs[a].at[l, 6, pl.ds(half, half)], 2, fwd_s.at[l, a], fwd_r.at[l, a]))

    def relay(l, a, i):
        src = (own[a], from_x[a], from_y[a])[i].at[l] if i < 3 else bufs[a].at[l, 6]
        return send(src, bufs[a].at[l, 2 * i + 1], 1, rel_s.at[l, a], rel_r.at[l, a])

    def forwards_wait(sems, l, a):
        pltpu.make_async_copy(bufs[a].at[l, 6], bufs[a].at[l, 6], sems.at[l, a]).wait()

    def relays_wait(sems, l, a):
        part = bufs[a].at[l, pl.ds(0, 4)]
        pltpu.make_async_copy(part, part, sems.at[l, a]).wait()

    def weights_start(l):
        for a in range(4):
            for c in forwards(l, a):
                c.start()
        for a in range(4):
            for i in range(3):
                relay(l, a, i).start()

    def weights_relay_last(l, a):
        forwards_wait(fwd_r, l, a)
        relay(l, a, 3).start()

    def weights_arrived(l, a):
        relays_wait(rel_r, l, a)

    ffw = (w_gate, w_up)
    ffbuf = (gbuf, ubuf)

    def unit_start(g, s):
        l, k = g // CHUNKS, lax.rem(g, CHUNKS)
        for m in PEERS:
            cols = pl.ds(pl.multiple_of(peer[m] * FF_BLOCK + k * CHUNK, CHUNK), CHUNK)
            send(ffw[s].at[l, :, cols], ffbuf[s].at[l, k, al(me, SHARD)], m, chunk_s.at[l, s], chunk_r.at[g, s]).start()

    last_g = LAYERS * CHUNKS - 1
    last_own = pltpu.make_async_copy(
        w_up.at[LAYERS - 1, :, pl.ds(pl.multiple_of(me * FF_BLOCK + (CHUNKS - 1) * CHUNK, CHUNK), CHUNK)], u_last.at[al(me, SHARD)], down_sem.at[1])
    last_own.start()

    def last_up_start():
        for m in PEERS:
            cols = pl.ds(pl.multiple_of(peer[m] * FF_BLOCK + (CHUNKS - 1) * CHUNK, CHUNK), CHUNK)
            send(w_up.at[LAYERS - 1, :, cols], u_last.at[al(me, SHARD)], m, chunk_s.at[LAYERS - 1, 1], chunk_r.at[last_g, 1]).start()

    def last_up_wait():
        last_own.wait()
        part = u_last.at[pl.ds(0, (WAYS - 1) * SHARD)]
        pltpu.make_async_copy(part, part, chunk_r.at[last_g, 1]).wait()

    def unit_wait(g, s):
        l, k = g // CHUNKS, lax.rem(g, CHUNKS)
        part = ffbuf[s].at[l, k, pl.ds(0, (WAYS - 1) * SHARD)]
        pltpu.make_async_copy(part, part, chunk_r.at[g, s]).wait()

    weights_start(0)

    gain_copies = [send(gains_own, gains_all.at[me], m, gain_s.at[0], gain_r.at[0]) for m in range(1, WAYS)]
    for c in gain_copies:
        c.start()

    @pl.loop(0, AHEAD)
    def _(g):
        unit_start(g, 0)
        unit_start(g, 1)

    def gains_wait(sem):
        part = gains_all.at[pl.ds(0, WAYS - 1)]
        pltpu.make_async_copy(part, part, sem.at[0]).wait()

    gains_wait(gain_r)

    def norm_into(src, gain_row, dst, dst_row0):
        @pl.loop(0, ROWS // 32)
        def _(i):
            h = src[al(i, 32), :].astype(F32)
            r = lax.rsqrt(jnp.mean(h * h, axis=-1, keepdims=True) + EPS)
            for s in range(WAYS):
                cols = pl.ds(s * SHARD, SHARD)
                g = 1.0 + gains_all[s, pl.ds(gain_row, 1), :]
                dst[pl.ds(pl.multiple_of(dst_row0 + i * 32, 32), 32), cols] = (h[:, s * SHARD:(s + 1) * SHARD] * r * g).astype(BF16)

    def tile_copies(l, a, n, slot):
        cols = al(n, HEAD)
        srcs = (own[a].at[l], bufs[a].at[l, 1], from_x[a].at[l], bufs[a].at[l, 3],
                from_y[a].at[l], bufs[a].at[l, 5], bufs[a].at[l, 6], bufs[a].at[l, 7])
        return [pltpu.make_async_copy(srcs[m].at[:, cols], w_tile.at[slot, al(peer[m], SHARD)], tile_sem.at[slot])
                for m in range(WAYS)]

    def tile_start(l, a, n, slot):
        for c in tile_copies(l, a, n, slot):
            c.start()

    def tile_wait(slot):
        pltpu.make_async_copy(w_tile.at[slot], w_tile.at[slot], tile_sem.at[slot]).wait()

    def rope(vec):
        lead, tail = vec[:, :HALF], vec[:, HALF:]
        cos_b, sin_b = cos_ref[...], sin_ref[...]
        return jnp.concatenate([lead * cos_b - tail * sin_b, tail * cos_b + lead * sin_b], axis=-1)

    def kv_copies(l, i, slot):
        return (pltpu.make_async_copy(k_cache.at[l, al(i, GROUP)], kv_k.at[slot], kv_sem.at[slot, 0]),
                pltpu.make_async_copy(v_cache.at[l, al(i, GROUP)], kv_v.at[slot], kv_sem.at[slot, 1]))

    def kv_start(l, i, slot):
        for c in kv_copies(l, i, slot):
            c.start()

    def attention_step(l, i):
        slot = lax.rem(i, 2)

        @pl.when(i + 1 < GROUPS)
        def _():
            kv_start(l, i + 1, 1 - slot)

        for c in kv_copies(l, i, slot):
            c.wait()
        rows = GROUP * HEADS
        q64 = q_seq[al(i, GROUP)].reshape(rows, HEAD)
        kn64 = jnp.broadcast_to(kn[al(i, GROUP), :][:, None, :], (GROUP, HEADS, HEAD)).reshape(rows, HEAD)
        vn64 = jnp.broadcast_to(vn[al(i, GROUP), :][:, None, :], (GROUP, HEADS, HEAD)).reshape(rows, HEAD)
        pos = pos_rep[al(i, rows), :]
        scores = jnp.concatenate(
            [lax.dot_general(q64[s * HEADS:(s + 1) * HEADS].astype(BF16), kv_k[slot, s], (((1,), (1,)), ((), ())), preferred_element_type=F32)
             for s in range(GROUP)], axis=0)
        new_score = jnp.sum(q64 * kn64, axis=-1, keepdims=True)
        place = lax.broadcasted_iota(jnp.int32, (rows, SMAX), 1)
        is_new = place == pos
        scores = jnp.where(is_new, new_score, scores)
        scores = jnp.where(place <= pos, scores, -1e30)
        u = jnp.exp(scores - jnp.max(scores, axis=-1, keepdims=True))
        den = jnp.sum(u, axis=-1, keepdims=True)
        u_new = jnp.sum(jnp.where(is_new, u, 0.0), axis=-1, keepdims=True).astype(BF16).astype(F32)
        u_old = jnp.where(is_new, 0.0, u)
        vals = jnp.concatenate(
            [jnp.dot(u_old[s * HEADS:(s + 1) * HEADS].astype(BF16), kv_v[slot, s], preferred_element_type=F32)
             for s in range(GROUP)], axis=0)
        vals = (vals + u_new * vn64) / den
        a_seq[al(i, GROUP)] = vals.reshape(GROUP, HEADS, HEAD)

    def y_wait(l, sem, rows):
        part = y_full.at[l, pl.ds(0, rows)]
        pltpu.make_async_copy(part, part, sem).wait()

    def y_send(l, m):
        mine = y_full.at[l, al(me, ROWS)]
        return send(mine, mine, m, y_s.at[l], y_r.at[l, m // 2])

    def y_forward(l, m):
        first = 0 if m == 2 else ROWS // 2
        block = y_full.at[l, pl.ds(pl.multiple_of(peer[m] * ROWS + first, ROWS // 2), ROWS // 2)]
        return send(block, block, 6 - m, y_s.at[l], y_r.at[l, 3])

    def y_relay(l, m):
        block = y_full.at[l, al(peer[m], ROWS)]
        return send(block, block, 1, y_s.at[l], y_r.at[l, 0])

    fftile = (g_tile, u_tile)

    def tile_in(l, k, s):
        unit_wait(l * CHUNKS + k, s)
        slot = lax.rem(k, 2)
        own_cols = pl.ds(pl.multiple_of(me * FF_BLOCK + k * CHUNK, CHUNK), CHUNK)
        for m in range(WAYS):
            src = ffw[s].at[l, :, own_cols] if m == 0 else ffbuf[s].at[l, k, al(peer[m], SHARD)]
            pltpu.make_async_copy(src, fftile[s].at[slot, al(peer[m], SHARD)], gate_sem.at[s, slot]).start()

    def tile_ready(k, s):
        slot = lax.rem(k, 2)
        pltpu.make_async_copy(fftile[s].at[slot], fftile[s].at[slot], gate_sem.at[s, slot]).wait()

    def mlp_chunk(l, k, last, down):
        slot = lax.rem(k, 2)
        d_copy = pltpu.make_async_copy(w_down.at[l, al(k, CHUNK)], d_tile, down_sem.at[0])
        d_copy.start()
        tile_ready(k, 0)
        if not last:
            tile_in(l, k, 1)

        @pl.loop(0, BATCH // MROWS)
        def _(i):
            gate = jnp.dot(y_full[l, al(i, MROWS), :], g_tile[slot], preferred_element_type=F32)
            gate_act[al(i, MROWS), :] = jax.nn.gelu(gate, approximate=True)

        direct = last and l == LAYERS - 1
        if direct:
            last_up_wait()
        else:
            if last:
                tile_in(l, k, 1)
            tile_ready(k, 1)

        @pl.loop(0, BATCH // MROWS)
        def _(i):
            u_cols = u_last[...] if direct else u_tile[slot]
            up = jnp.dot(y_full[l, al(i, MROWS), :], u_cols, preferred_element_type=F32)
            m_act[al(i, MROWS), :] = (gate_act[al(i, MROWS), :] * up).astype(BF16)

        if not last:
            tile_in(l, k + 1, 0)
        d_copy.wait()
        down()

    def down_piece(cols, first):
        @pl.loop(0, BATCH // DROWS)
        def _(i):
            part = jnp.dot(m_act[al(i, DROWS), :], d_tile[:, cols], preferred_element_type=F32)
            for b in range(DROWS // ROWS):
                blk = i * (DROWS // ROWS) + b
                piece = part[b * ROWS:(b + 1) * ROWS]
                acc[blk, :, cols] = piece if first else acc[blk, :, cols] + piece

    half_d = D // 2

    def piece(s):
        start, width = PIECES[s]
        return start < half_d, pl.ds(start, width), pl.ds(start % half_d, width)

    def rs_core(s):
        _, cols, _ = piece(s)
        return [send(acc.at[2 * j + 1 - core, :, cols], core_recv.at[j, :, cols], 1, rs_s.at[0, s], rs_r.at[0, s]) for j in range(4)]

    def rs_first(s):
        left, cols, local = piece(s)
        if left:
            return [send(acc.at[2 * (2 * t + 1 - xbit) + core, :, cols], p1a.at[t, :, local], 2, rs_s.at[1, s], rs_r.at[1, s]) for t in range(2)]
        return [send(acc.at[2 * (2 * (1 - ybit) + t) + core, :, cols], p1b.at[t, :, local], 4, rs_s.at[1, s], rs_r.at[1, s]) for t in range(2)]

    def rs_second(s):
        left, cols, local = piece(s)
        if left:
            return [send(acc.at[2 * (2 * (1 - ybit) + xbit) + core, :, cols], p2a.at[:, local], 4, rs_s.at[2, s], rs_r.at[2, s])]
        return [send(acc.at[2 * (2 * ybit + 1 - xbit) + core, :, cols], p2b.at[:, local], 2, rs_s.at[2, s], rs_r.at[2, s])]

    def rs_wait(sems, phase, s):
        left, cols, local = piece(s)
        ref = (core_recv.at[:, :, cols], (p1a if left else p1b).at[:, :, local], (p2a if left else p2b).at[:, local])[phase]
        pltpu.make_async_copy(ref, ref, sems.at[phase, s]).wait()

    def rs_core_add(s):
        _, cols, _ = piece(s)
        rs_wait(rs_r, 0, s)

        @pl.loop(0, 4)
        def _(j):
            acc[2 * j + core, :, cols] = acc[2 * j + core, :, cols] + core_recv[j, :, cols]

    def rs_first_add(s):
        left, cols, local = piece(s)
        rs_wait(rs_r, 1, s)

        @pl.loop(0, 2)
        def _(t):
            if left:
                blk = 2 * (2 * t + xbit) + core
                acc[blk, :, cols] = acc[blk, :, cols] + p1a[t, :, local]
            else:
                blk = 2 * (2 * ybit + t) + core
                acc[blk, :, cols] = acc[blk, :, cols] + p1b[t, :, local]

    def rs_second_add(s):
        left, cols, local = piece(s)
        rs_wait(rs_r, 2, s)
        other = p2a[:, local] if left else p2b[:, local]
        total = acc[me, :, cols] + other
        hid[:, cols] = (hid[:, cols].astype(F32) + total).astype(BF16)

    def slab_in(l):
        return (pltpu.make_async_copy(k_slabs.at[l], k_slab.at[l], slab_sem.at[l, 0]),
                pltpu.make_async_copy(v_slabs.at[l], v_slab.at[l], slab_sem.at[l, 1]))

    def slab_out(l):
        return (pltpu.make_async_copy(k_slab.at[l], k_slabs_out.at[l], slab_sem.at[l, 2]),
                pltpu.make_async_copy(v_slab.at[l], v_slabs_out.at[l], slab_sem.at[l, 3]))

    def slab_fill(l):
        for c in slab_in(l):
            c.wait()
        row = lax.broadcasted_iota(jnp.int32, (SLAB, HEAD), 0)

        @pl.loop(0, GROUPS)
        def _(i):
            k8 = kn[al(i, GROUP), :]
            v8 = vn[al(i, GROUP), :]
            pos = pos_rep[al(i, GROUP * HEADS), :]
            for j in range(GROUP):
                q = i * GROUP + j
                hit = row == jnp.bitwise_and(pos[j * HEADS:j * HEADS + 1], SLAB - 1)
                k_slab[l, q] = jnp.where(hit, k8[j:j + 1], k_slab[l, q].astype(F32)).astype(BF16)
                v_slab[l, q] = jnp.where(hit, v8[j:j + 1], v_slab[l, q].astype(F32)).astype(BF16)

        for c in slab_out(l):
            c.start()

    order = range(len(PIECES))

    def hid_store(s):
        cols = pl.ds(*PIECES[s])
        return pltpu.make_async_copy(hid.at[:, cols], hid_out.at[:, cols], store_sem.at[s])

    def sends_over():
        gains_wait(gain_s)
        for l in range(LAYERS):
            for a in range(4):
                forwards_wait(fwd_s, l, a)
                relays_wait(rel_s, l, a)
            y_wait(l, y_s.at[l], 7 * ROWS)

        for l in range(LAYERS):
            for s in range(2):
                part = ffbuf[s].at[l, pl.ds(0, CHUNKS * (WAYS - 1) // WAYS)]
                pltpu.make_async_copy(part, part, chunk_s.at[l, s]).wait()

        for l in range(LAYERS):
            for c in slab_out(l):
                c.wait()

    for l in range(LAYERS):
        for c in slab_in(l):
            c.start()

    for c in loads:
        c.wait()

    for l in range(LAYERS):
        base = l * CHUNKS
        norm_into(hid, l, x_act, 0)
        if l == 0:
            for a in range(3):
                weights_relay_last(l, a)
        kv_start(l, 0, 0)
        for a in range(3):
            weights_arrived(l, a)
        tile_start(l, 0, 0, 0)

        @pl.loop(0, HEADS)
        def _(h, l=l):
            slot = lax.rem(h, 2)

            @pl.when(h + 1 < HEADS)
            def _():
                tile_start(l, 0, h + 1, 1 - slot)

            tile_wait(slot)
            q = rope(jnp.dot(x_act[...], w_tile[slot], preferred_element_type=F32))
            q_head[h] = (q * HEAD ** -0.5).astype(BF16).astype(F32)

        tile_start(l, 1, 0, 0)
        tile_start(l, 2, 0, 1)
        for h in range(HEADS):
            q_seq[:, h, :] = q_head[h]
        tile_wait(0)
        kn[...] = rope(jnp.dot(x_act[...], w_tile[0], preferred_element_type=F32)).astype(BF16).astype(F32)
        tile_wait(1)
        vn[...] = jnp.dot(x_act[...], w_tile[1], preferred_element_type=F32).astype(BF16).astype(F32)

        if l == 0:
            weights_relay_last(l, 3)
        else:
            unit_start(base + 2, 0)

        @pl.loop(0, GROUPS // 2)
        def _(i, l=l):
            attention_step(l, i)

        unit_start(base + 2, l)

        @pl.loop(GROUPS // 2, GROUPS)
        def _(i, l=l):
            attention_step(l, i)

        if l == 0:
            unit_start(base + 2, 1)
        for h in range(HEADS):
            a_flat[:, pl.ds(h * HEAD, HEAD)] = a_seq[:, h, :].astype(BF16)
        weights_arrived(l, 3)
        tile_start(l, 3, 0, 0)

        @pl.loop(0, HEADS)
        def _(n, l=l):
            slot = lax.rem(n, 2)

            @pl.when(n + 1 < HEADS)
            def _():
                tile_start(l, 3, n + 1, 1 - slot)

            tile_wait(slot)
            cols = al(n, HEAD)
            part = jnp.dot(a_flat[...], w_tile[slot], preferred_element_type=F32)
            hid[:, cols] = (hid[:, cols].astype(F32) + part).astype(BF16)

        norm_into(hid, LAYERS + l, y_full.at[l], me * ROWS)
        for m in (2, 4, 1):
            y_send(l, m).start()
        unit_start(base + 3, 0)
        for m in (2, 4):
            y_send(l, m).wait_recv()
            y_forward(l, m).start()
        unit_start(base + 3, 1)
        for m in (2, 4):
            y_relay(l, m).start()
        y_wait(l, y_r.at[l, 3], ROWS)
        y_relay(l, 6).start()
        y_wait(l, y_r.at[l, 0], 4 * ROWS)

        if l == 0:
            weights_start(1)

        @pl.loop(base + 4, base + CHUNKS - l)
        def _(g):
            unit_start(g, 0)
            unit_start(g, 1)

        if l == LAYERS - 1:
            unit_start(last_g, 0)
            last_up_start()

        def first_down():
            @pl.loop(0, D // SUB)
            def _(s):
                down_piece(al(s, SUB), True)

        def more_down():
            @pl.loop(0, D // SUB)
            def _(s):
                down_piece(al(s, SUB), False)

        tile_in(l, 0, 0)
        mlp_chunk(l, 0, False, first_down)

        @pl.loop(1, CHUNKS - 1)
        def _(k, l=l):
            mlp_chunk(l, k, False, more_down)

        if l == 0:
            for a in range(4):
                weights_relay_last(1, a)
            unit_start(CHUNKS, 0)

        def last_down():
            for s in order:
                down_piece(pl.ds(*PIECES[s]), False)
                for c in rs_core(s):
                    c.start()

        mlp_chunk(l, CHUNKS - 1, True, last_down)
        for s in order:
            rs_core_add(s)
            for c in rs_first(s):
                c.start()
        if l == 0:
            unit_start(CHUNKS, 1)
        slab_fill(l)
        if l == LAYERS - 1:
            sends_over()
        for s in order:
            rs_first_add(s)
            for c in rs_second(s):
                c.start()
        if l == 0:
            unit_start(CHUNKS + 1, 0)
            unit_start(CHUNKS + 1, 1)
        for s in order:
            rs_second_add(s)
            if l == LAYERS - 1:
                hid_store(s).start()
        if l == 0:
            for s in order:
                for phase in range(3):
                    rs_wait(rs_s, phase, s)

    for s in order:
        hid_store(s).wait()
        for phase in range(3):
            rs_wait(rs_s, phase, s)


def run_layers(*operands):
    any_spec = pl.BlockSpec(memory_space=pl.ANY)
    sds = jax.ShapeDtypeStruct
    dma = pltpu.SemaphoreType.DMA
    return pl.pallas_call(
        layers_kernel,
        name="layers",
        out_shape=[
            sds((ROWS, D), BF16), sds((LAYERS, ROWS, SLAB, HEAD), BF16), sds((LAYERS, ROWS, SLAB, HEAD), BF16),
            sds((LAYERS, WAYS, SHARD, D), BF16), sds((LAYERS, WAYS, SHARD, HEAD), BF16),
            sds((LAYERS, WAYS, SHARD, HEAD), BF16), sds((LAYERS, WAYS, SHARD, D), BF16),
            sds((LAYERS, CHUNKS, D, CHUNK), BF16), sds((LAYERS, CHUNKS, D, CHUNK), BF16),
        ],
        in_specs=[any_spec] * 24,
        out_specs=[any_spec] * 9,
        scratch_shapes=[
            pltpu.VMEM((WAYS, 8, SHARD), F32),
            pltpu.VMEM((ROWS, D), BF16),
            pltpu.VMEM((ROWS, D), BF16),
            pltpu.VMEM((HEADS, ROWS, HEAD), F32),
            pltpu.VMEM((ROWS, HEADS, HEAD), F32),
            pltpu.VMEM((ROWS, HEADS, HEAD), F32),
            pltpu.VMEM((ROWS, D), BF16),
            pltpu.VMEM((ROWS, HEAD), F32),
            pltpu.VMEM((ROWS, HEAD), F32),
            pltpu.VMEM((2, GROUP, SMAX, HEAD), BF16),
            pltpu.VMEM((2, GROUP, SMAX, HEAD), BF16),
            pltpu.VMEM((2, D, HEAD), BF16),
            pltpu.VMEM((LAYERS, BATCH, D), BF16),
            pltpu.VMEM((2, D, CHUNK), BF16),
            pltpu.VMEM((2, D, CHUNK), BF16),
            pltpu.VMEM((BATCH, CHUNK), F32),
            pltpu.VMEM((CHUNK, D), BF16),
            pltpu.VMEM((BATCH, CHUNK), BF16),
            pltpu.VMEM((WAYS, ROWS, D), F32),
            pltpu.VMEM((4, ROWS, D), F32),
            pltpu.VMEM((2, ROWS, D // 2), F32),
            pltpu.VMEM((2, ROWS, D // 2), F32),
            pltpu.VMEM((ROWS, D // 2), F32),
            pltpu.VMEM((ROWS, D // 2), F32),
            pltpu.VMEM((LAYERS, ROWS, SLAB, HEAD), BF16),
            pltpu.VMEM((LAYERS, ROWS, SLAB, HEAD), BF16),
            pltpu.VMEM((D, CHUNK), BF16),
            pltpu.VMEM((BATCH, 1), jnp.int32),
            pltpu.VMEM((ROWS, HALF), F32),
            pltpu.VMEM((ROWS, HALF), F32),
            dma((1,)), dma((1,)),
            dma((LAYERS, 4)), dma((LAYERS, 4)),
            dma((LAYERS, 4)), dma((LAYERS, 4)),
            dma((LAYERS, 2)), dma((LAYERS * CHUNKS, 2)),
            dma((LAYERS,)), dma((LAYERS, 4)),
            dma((3, len(PIECES))), dma((3, len(PIECES))),
            dma((2,)), dma((2, 2)), dma((2, 2)), dma((2,)), dma((LAYERS, 4)), dma((5,)), dma((len(PIECES),)),
        ],
        compiler_params=pltpu.CompilerParams(collective_id=0, has_side_effects=True, vmem_limit_bytes=63 * 2**20),
        cost_estimate=pl.CostEstimate(flops=60 * 10**9, bytes_accessed=300 * 10**6, transcendentals=0),
    )(*operands)


COPY_ROWS = 16


def slab_base(positions, s):
    return pl.multiple_of((positions[s] // SLAB) * SLAB, SLAB)


def copy_kernel(positions, k_in, v_in, k_out, v_out, k_slabs, v_slabs):
    k_out[...] = k_in[...]
    v_out[...] = v_in[...]
    first = pl.program_id(1) * COPY_ROWS
    for j in range(COPY_ROWS):
        base = slab_base(positions, first + j)
        k_slabs[0, j] = k_in[0, j, pl.ds(base, SLAB), :]
        v_slabs[0, j] = v_in[0, j, pl.ds(base, SLAB), :]


def copy_caches(positions, k_cache, v_cache):
    spec = pl.BlockSpec((1, COPY_ROWS, SMAX, HEAD), lambda l, i: (l, i, 0, 0))
    slab_spec = pl.BlockSpec((1, COPY_ROWS, SLAB, HEAD), lambda l, i: (l, i, 0, 0))
    shape = jax.ShapeDtypeStruct(k_cache.shape, k_cache.dtype)
    slab_shape = jax.ShapeDtypeStruct((LAYERS, ROWS, SLAB, HEAD), k_cache.dtype)
    return pl.pallas_call(
        copy_kernel, name="copy_caches", grid=(LAYERS, ROWS // COPY_ROWS),
        in_specs=[pl.BlockSpec(memory_space=pltpu.SMEM), spec, spec], out_specs=[spec, spec, slab_spec, slab_spec],
        out_shape=[shape, shape, slab_shape, slab_shape],
        compiler_params=pltpu.CompilerParams(vmem_limit_bytes=40 * 2**20),
        cost_estimate=pl.CostEstimate(flops=20 * 10**9, bytes_accessed=4 * k_cache.size * 2, transcendentals=0),
    )(positions, k_cache, v_cache)


def place_kernel(positions, hid_in, k_slabs, v_slabs, k_in, v_in, hid_out, k_out, v_out, hid, k_slab, v_slab, sems):
    def place(ref, s):
        return ref.at[:, s, pl.ds(slab_base(positions, s), SLAB), :]

    ins = [pltpu.make_async_copy(src.at[l], dst.at[l], sems.at[0, 2 * l + i])
           for l in range(LAYERS) for i, (src, dst) in enumerate(((k_slabs, k_slab), (v_slabs, v_slab)))]
    for c in ins:
        c.start()
    hid_load = pltpu.make_async_copy(hid_in, hid, sems.at[1, 2])
    hid_load.start()
    for c in ins:
        c.wait()

    @pl.loop(0, ROWS // 4)
    def _(i):
        for j in range(4):
            s = i * 4 + j
            pltpu.make_async_copy(k_slab.at[:, s], place(k_out, s), sems.at[1, 0]).start()
            pltpu.make_async_copy(v_slab.at[:, s], place(v_out, s), sems.at[1, 1]).start()

    hid_load.wait()
    hid_store = pltpu.make_async_copy(hid, hid_out, sems.at[1, 3])
    hid_store.start()
    pltpu.make_async_copy(k_slab, k_slab, sems.at[1, 0]).wait()
    pltpu.make_async_copy(v_slab, v_slab, sems.at[1, 1]).wait()
    hid_store.wait()


def place_rows(positions, hidden, k_slabs, v_slabs, k_copy, v_copy):
    any_spec = pl.BlockSpec(memory_space=pl.ANY)
    shape = jax.ShapeDtypeStruct(k_copy.shape, k_copy.dtype)
    slab = pltpu.VMEM((LAYERS, ROWS, SLAB, HEAD), BF16)
    return pl.pallas_call(
        place_kernel, name="place_rows",
        in_specs=[pl.BlockSpec(memory_space=pltpu.SMEM)] + [any_spec] * 5,
        out_specs=[any_spec] * 3, out_shape=[jax.ShapeDtypeStruct(hidden.shape, hidden.dtype), shape, shape], input_output_aliases={4: 1, 5: 2},
        scratch_shapes=[pltpu.VMEM((ROWS, D), BF16), slab, slab, pltpu.SemaphoreType.DMA((2, 4))],
        compiler_params=pltpu.CompilerParams(vmem_limit_bytes=63 * 2**20),
    )(positions, hidden, k_slabs, v_slabs, k_copy, v_copy)


def solution(mesh):
    batch_spec = P(("dp", "w"))
    cache_spec = P(None, ("dp", "w"))
    gain_spec = P(None, "w")
    weight_spec = P(None, "w", None)
    x_swap = [(s, s ^ 2) for s in range(WAYS)]
    y_swap = [(s, s ^ 4) for s in range(WAYS)]

    def per_device(hidden, positions, k_cache, v_cache, attn_norm, w_query, w_key, w_value, w_out, mlp_norm, w_gate, w_up, w_down):
        attn_weights = (w_query, w_key, w_value, w_out)
        from_x = tuple(lax.ppermute(w, "w", x_swap) for w in attn_weights)
        from_y = tuple(lax.ppermute(w, "w", y_swap) for w in attn_weights)
        cos_tab, sin_tab = rope_tables(positions)
        pos_rep = jnp.repeat(positions, HEADS)[:, None]
        gains = jnp.concatenate([attn_norm, mlp_norm, attn_norm, mlp_norm], axis=0)
        k_in, v_in, cos_tab, sin_tab, pos_rep, gains = lax.optimization_barrier((k_cache[:, :, 0], v_cache[:, :, 0], cos_tab, sin_tab, pos_rep, gains))
        k_copy, v_copy, k_slabs, v_slabs = copy_caches(positions, k_in, v_in)
        outs = run_layers(hidden, pos_rep, cos_tab, sin_tab, gains, k_copy, v_copy, k_slabs, v_slabs, *attn_weights, *from_x, *from_y, w_gate, w_up, w_down)
        hidden_out, k_out, v_out = place_rows(positions, outs[0], outs[1], outs[2], k_copy, v_copy)
        return hidden_out, k_out[:, :, None], v_out[:, :, None]

    in_specs = (batch_spec, batch_spec, cache_spec, cache_spec, gain_spec, weight_spec, weight_spec, weight_spec, weight_spec, gain_spec, weight_spec, weight_spec, weight_spec)
    out_specs = (batch_spec, cache_spec, cache_spec)
    return jax.shard_map(per_device, mesh=mesh, in_specs=in_specs, out_specs=out_specs, check_vma=False)
```

```python
import jax
import jax.numpy as jnp
from jax import lax
from jax.experimental import pallas as pl
from jax.experimental.pallas import tpu as pltpu
from jax.sharding import PartitionSpec as P

EPS = 1e-6
ROPE_BASE = 10000.0
MESH = pl.DeviceIdType.MESH
BF16 = jnp.bfloat16
F32 = jnp.float32

WAYS = 8
LAYERS = 2
ROWS = 128
BATCH = ROWS * WAYS
D = 2048
SHARD = D // WAYS
HEADS = 8
HEAD = 256
HALF = HEAD // 2
SMAX = 256
FF_BLOCK = 2048
CHUNK = 256
CHUNKS = FF_BLOCK // CHUNK
GROUP = 8
GROUPS = ROWS // GROUP
SUB = 512
PIECES = ((0, 128), (1024, 128), (128, 640), (1152, 640), (768, 256), (1792, 256))
SLAB = 16
PEERS = (6, 7, 2, 4, 3, 5, 1)
AHEAD = 2
MROWS = 512
DROWS = 512


def rope_tables(positions):
    inv_freq = ROPE_BASE ** (-2.0 * jnp.arange(HALF, dtype=F32) / HEAD)
    angles = positions.astype(F32)[:, None] * inv_freq[None, :]
    return jnp.cos(angles), jnp.sin(angles)


def al(index, size):
    return pl.ds(pl.multiple_of(index * size, size), size)


def layers_kernel(hid_in, pos_in, cos_in, sin_in, gains_own, k_cache, v_cache, k_slabs, v_slabs,
                  wq, wk, wv, wo, qx, kx, vx, ox, qy, ky, vy, oy, w_gate, w_up, w_down,
                  hid_out, k_slabs_out, v_slabs_out, qbuf, kbuf, vbuf, obuf, gbuf, ubuf,
                  gains_all, hid, x_act, q_head, q_seq, a_seq, a_flat, kn, vn, kv_k, kv_v, w_tile,
                  y_full, g_tile, u_tile, gate_act, d_tile, m_act, acc, core_recv, p1a, p1b, p2a, p2b, k_slab, v_slab, u_last, pos_rep, cos_ref, sin_ref,
                  gain_s, gain_r, fwd_s, fwd_r, rel_s, rel_r, chunk_s, chunk_r, y_s, y_r,
                  rs_s, rs_r, tile_sem, kv_sem, gate_sem, down_sem, slab_sem, load_sem, store_sem):
    me = lax.axis_index("w")
    core = lax.rem(me, 2)
    xbit = lax.rem(me // 2, 2)
    ybit = me // 4
    peer = [jnp.bitwise_xor(me, m) for m in range(WAYS)]

    def send(src, dst, m, ssem, rsem):
        return pltpu.make_async_remote_copy(src_ref=src, dst_ref=dst, send_sem=ssem, recv_sem=rsem,
                                            device_id={"w": peer[m]}, device_id_type=MESH)

    loads = [pltpu.make_async_copy(src, dst, load_sem.at[i]) for i, (src, dst) in enumerate((
        (gains_own, gains_all.at[me]), (hid_in, hid), (cos_in, cos_ref), (sin_in, sin_ref), (pos_in, pos_rep)))]
    for c in loads:
        c.start()

    barrier = pltpu.get_barrier_semaphore()
    for m in range(1, WAYS):
        pl.semaphore_signal(barrier, inc=1, device_id={"w": peer[m]}, device_id_type=MESH)
    pl.semaphore_wait(barrier, WAYS - 1)

    own = (wq, wk, wv, wo)
    from_x = (qx, kx, vx, ox)
    from_y = (qy, ky, vy, oy)
    bufs = (qbuf, kbuf, vbuf, obuf)
    half = SHARD // 2

    def forwards(l, a):
        return (send(from_x[a].at[l, pl.ds(0, half)], bufs[a].at[l, 6, pl.ds(0, half)], 4, fwd_s.at[l, a], fwd_r.at[l, a]),
                send(from_y[a].at[l, pl.ds(half, half)], bufs[a].at[l, 6, pl.ds(half, half)], 2, fwd_s.at[l, a], fwd_r.at[l, a]))

    def relay(l, a, i):
        src = (own[a], from_x[a], from_y[a])[i].at[l] if i < 3 else bufs[a].at[l, 6]
        return send(src, bufs[a].at[l, 2 * i + 1], 1, rel_s.at[l, a], rel_r.at[l, a])

    def forwards_wait(sems, l, a):
        pltpu.make_async_copy(bufs[a].at[l, 6], bufs[a].at[l, 6], sems.at[l, a]).wait()

    def relays_wait(sems, l, a):
        part = bufs[a].at[l, pl.ds(0, 4)]
        pltpu.make_async_copy(part, part, sems.at[l, a]).wait()

    def weights_start(l):
        for a in range(4):
            for c in forwards(l, a):
                c.start()
        for a in range(4):
            for i in range(3):
                relay(l, a, i).start()

    def weights_relay_last(l, a):
        forwards_wait(fwd_r, l, a)
        relay(l, a, 3).start()

    def weights_arrived(l, a):
        relays_wait(rel_r, l, a)

    ffw = (w_gate, w_up)
    ffbuf = (gbuf, ubuf)

    def unit_start(g, s):
        l, k = g // CHUNKS, lax.rem(g, CHUNKS)
        for m in PEERS:
            cols = pl.ds(pl.multiple_of(peer[m] * FF_BLOCK + k * CHUNK, CHUNK), CHUNK)
            send(ffw[s].at[l, :, cols], ffbuf[s].at[l, k, al(me, SHARD)], m, chunk_s.at[l, s], chunk_r.at[g, s]).start()

    last_g = LAYERS * CHUNKS - 1
    last_own = pltpu.make_async_copy(
        w_up.at[LAYERS - 1, :, pl.ds(pl.multiple_of(me * FF_BLOCK + (CHUNKS - 1) * CHUNK, CHUNK), CHUNK)], u_last.at[al(me, SHARD)], down_sem.at[1])
    last_own.start()

    def last_up_start():
        for m in PEERS:
            cols = pl.ds(pl.multiple_of(peer[m] * FF_BLOCK + (CHUNKS - 1) * CHUNK, CHUNK), CHUNK)
            send(w_up.at[LAYERS - 1, :, cols], u_last.at[al(me, SHARD)], m, chunk_s.at[LAYERS - 1, 1], chunk_r.at[last_g, 1]).start()

    def last_up_wait():
        last_own.wait()
        part = u_last.at[pl.ds(0, (WAYS - 1) * SHARD)]
        pltpu.make_async_copy(part, part, chunk_r.at[last_g, 1]).wait()

    def unit_wait(g, s):
        l, k = g // CHUNKS, lax.rem(g, CHUNKS)
        part = ffbuf[s].at[l, k, pl.ds(0, (WAYS - 1) * SHARD)]
        pltpu.make_async_copy(part, part, chunk_r.at[g, s]).wait()

    weights_start(0)

    gain_copies = [send(gains_own, gains_all.at[me], m, gain_s.at[0], gain_r.at[0]) for m in range(1, WAYS)]
    for c in gain_copies:
        c.start()

    @pl.loop(0, AHEAD)
    def _(g):
        unit_start(g, 0)
        unit_start(g, 1)

    def gains_wait(sem):
        part = gains_all.at[pl.ds(0, WAYS - 1)]
        pltpu.make_async_copy(part, part, sem.at[0]).wait()

    gains_wait(gain_r)

    def norm_into(src, gain_row, dst, dst_row0):
        @pl.loop(0, ROWS // 32)
        def _(i):
            h = src[al(i, 32), :].astype(F32)
            r = lax.rsqrt(jnp.mean(h * h, axis=-1, keepdims=True) + EPS)
            for s in range(WAYS):
                cols = pl.ds(s * SHARD, SHARD)
                g = 1.0 + gains_all[s, pl.ds(gain_row, 1), :]
                dst[pl.ds(pl.multiple_of(dst_row0 + i * 32, 32), 32), cols] = (h[:, s * SHARD:(s + 1) * SHARD] * r * g).astype(BF16)

    def tile_copies(l, a, n, slot):
        cols = al(n, HEAD)
        srcs = (own[a].at[l], bufs[a].at[l, 1], from_x[a].at[l], bufs[a].at[l, 3],
                from_y[a].at[l], bufs[a].at[l, 5], bufs[a].at[l, 6], bufs[a].at[l, 7])
        return [pltpu.make_async_copy(srcs[m].at[:, cols], w_tile.at[slot, al(peer[m], SHARD)], tile_sem.at[slot])
                for m in range(WAYS)]

    def tile_start(l, a, n, slot):
        for c in tile_copies(l, a, n, slot):
            c.start()

    def tile_wait(slot):
        pltpu.make_async_copy(w_tile.at[slot], w_tile.at[slot], tile_sem.at[slot]).wait()

    def rope(vec):
        lead, tail = vec[:, :HALF], vec[:, HALF:]
        cos_b, sin_b = cos_ref[...], sin_ref[...]
        return jnp.concatenate([lead * cos_b - tail * sin_b, tail * cos_b + lead * sin_b], axis=-1)

    def kv_copies(l, i, slot):
        return (pltpu.make_async_copy(k_cache.at[l, al(i, GROUP)], kv_k.at[slot], kv_sem.at[slot, 0]),
                pltpu.make_async_copy(v_cache.at[l, al(i, GROUP)], kv_v.at[slot], kv_sem.at[slot, 1]))

    def kv_start(l, i, slot):
        for c in kv_copies(l, i, slot):
            c.start()

    def attention_step(l, i):
        slot = lax.rem(i, 2)

        @pl.when(i + 1 < GROUPS)
        def _():
            kv_start(l, i + 1, 1 - slot)

        for c in kv_copies(l, i, slot):
            c.wait()
        rows = GROUP * HEADS
        q64 = q_seq[al(i, GROUP)].reshape(rows, HEAD)
        kn64 = jnp.broadcast_to(kn[al(i, GROUP), :][:, None, :], (GROUP, HEADS, HEAD)).reshape(rows, HEAD)
        vn64 = jnp.broadcast_to(vn[al(i, GROUP), :][:, None, :], (GROUP, HEADS, HEAD)).reshape(rows, HEAD)
        pos = pos_rep[al(i, rows), :]
        scores = jnp.concatenate(
            [lax.dot_general(q64[s * HEADS:(s + 1) * HEADS].astype(BF16), kv_k[slot, s], (((1,), (1,)), ((), ())), preferred_element_type=F32)
             for s in range(GROUP)], axis=0)
        new_score = jnp.sum(q64 * kn64, axis=-1, keepdims=True)
        place = lax.broadcasted_iota(jnp.int32, (rows, SMAX), 1)
        is_new = place == pos
        scores = jnp.where(is_new, new_score, scores)
        scores = jnp.where(place <= pos, scores, -1e30)
        u = jnp.exp(scores - jnp.max(scores, axis=-1, keepdims=True))
        den = jnp.sum(u, axis=-1, keepdims=True)
        u_new = jnp.sum(jnp.where(is_new, u, 0.0), axis=-1, keepdims=True).astype(BF16).astype(F32)
        u_old = jnp.where(is_new, 0.0, u)
        vals = jnp.concatenate(
            [jnp.dot(u_old[s * HEADS:(s + 1) * HEADS].astype(BF16), kv_v[slot, s], preferred_element_type=F32)
             for s in range(GROUP)], axis=0)
        vals = (vals + u_new * vn64) / den
        a_seq[al(i, GROUP)] = vals.reshape(GROUP, HEADS, HEAD)

    def y_wait(l, sem, rows):
        part = y_full.at[l, pl.ds(0, rows)]
        pltpu.make_async_copy(part, part, sem).wait()

    def y_send(l, m):
        mine = y_full.at[l, al(me, ROWS)]
        return send(mine, mine, m, y_s.at[l], y_r.at[l, m // 2])

    def y_forward(l, m):
        first = 0 if m == 2 else ROWS // 2
        block = y_full.at[l, pl.ds(pl.multiple_of(peer[m] * ROWS + first, ROWS // 2), ROWS // 2)]
        return send(block, block, 6 - m, y_s.at[l], y_r.at[l, 3])

    def y_relay(l, m):
        block = y_full.at[l, al(peer[m], ROWS)]
        return send(block, block, 1, y_s.at[l], y_r.at[l, 0])

    fftile = (g_tile, u_tile)

    def tile_in(l, k, s):
        unit_wait(l * CHUNKS + k, s)
        slot = lax.rem(k, 2)
        own_cols = pl.ds(pl.multiple_of(me * FF_BLOCK + k * CHUNK, CHUNK), CHUNK)
        for m in range(WAYS):
            src = ffw[s].at[l, :, own_cols] if m == 0 else ffbuf[s].at[l, k, al(peer[m], SHARD)]
            pltpu.make_async_copy(src, fftile[s].at[slot, al(peer[m], SHARD)], gate_sem.at[s, slot]).start()

    def tile_ready(k, s):
        slot = lax.rem(k, 2)
        pltpu.make_async_copy(fftile[s].at[slot], fftile[s].at[slot], gate_sem.at[s, slot]).wait()

    def mlp_chunk(l, k, last, down):
        slot = lax.rem(k, 2)
        d_copy = pltpu.make_async_copy(w_down.at[l, al(k, CHUNK)], d_tile, down_sem.at[0])
        d_copy.start()
        tile_ready(k, 0)
        if not last:
            tile_in(l, k, 1)

        @pl.loop(0, BATCH // MROWS)
        def _(i):
            gate = jnp.dot(y_full[l, al(i, MROWS), :], g_tile[slot], preferred_element_type=F32)
            gate_act[al(i, MROWS), :] = jax.nn.gelu(gate, approximate=True)

        direct = last and l == LAYERS - 1
        if direct:
            last_up_wait()
        else:
            if last:
                tile_in(l, k, 1)
            tile_ready(k, 1)

        @pl.loop(0, BATCH // MROWS)
        def _(i):
            u_cols = u_last[...] if direct else u_tile[slot]
            up = jnp.dot(y_full[l, al(i, MROWS), :], u_cols, preferred_element_type=F32)
            m_act[al(i, MROWS), :] = (gate_act[al(i, MROWS), :] * up).astype(BF16)

        if not last:
            tile_in(l, k + 1, 0)
        d_copy.wait()
        down()

    def down_piece(cols, first):
        @pl.loop(0, BATCH // DROWS)
        def _(i):
            part = jnp.dot(m_act[al(i, DROWS), :], d_tile[:, cols], preferred_element_type=F32)
            for b in range(DROWS // ROWS):
                blk = i * (DROWS // ROWS) + b
                piece = part[b * ROWS:(b + 1) * ROWS]
                acc[blk, :, cols] = piece if first else acc[blk, :, cols] + piece

    half_d = D // 2

    def piece(s):
        start, width = PIECES[s]
        return start < half_d, pl.ds(start, width), pl.ds(start % half_d, width)

    def rs_core(s):
        _, cols, _ = piece(s)
        return [send(acc.at[2 * j + 1 - core, :, cols], core_recv.at[j, :, cols], 1, rs_s.at[0, s], rs_r.at[0, s]) for j in range(4)]

    def rs_first(s):
        left, cols, local = piece(s)
        if left:
            return [send(acc.at[2 * (2 * t + 1 - xbit) + core, :, cols], p1a.at[t, :, local], 2, rs_s.at[1, s], rs_r.at[1, s]) for t in range(2)]
        return [send(acc.at[2 * (2 * (1 - ybit) + t) + core, :, cols], p1b.at[t, :, local], 4, rs_s.at[1, s], rs_r.at[1, s]) for t in range(2)]

    def rs_second(s):
        left, cols, local = piece(s)
        if left:
            return [send(acc.at[2 * (2 * (1 - ybit) + xbit) + core, :, cols], p2a.at[:, local], 4, rs_s.at[2, s], rs_r.at[2, s])]
        return [send(acc.at[2 * (2 * ybit + 1 - xbit) + core, :, cols], p2b.at[:, local], 2, rs_s.at[2, s], rs_r.at[2, s])]

    def rs_wait(sems, phase, s):
        left, cols, local = piece(s)
        ref = (core_recv.at[:, :, cols], (p1a if left else p1b).at[:, :, local], (p2a if left else p2b).at[:, local])[phase]
        pltpu.make_async_copy(ref, ref, sems.at[phase, s]).wait()

    def rs_core_add(s):
        _, cols, _ = piece(s)
        rs_wait(rs_r, 0, s)

        @pl.loop(0, 4)
        def _(j):
            acc[2 * j + core, :, cols] = acc[2 * j + core, :, cols] + core_recv[j, :, cols]

    def rs_first_add(s):
        left, cols, local = piece(s)
        rs_wait(rs_r, 1, s)

        @pl.loop(0, 2)
        def _(t):
            if left:
                blk = 2 * (2 * t + xbit) + core
                acc[blk, :, cols] = acc[blk, :, cols] + p1a[t, :, local]
            else:
                blk = 2 * (2 * ybit + t) + core
                acc[blk, :, cols] = acc[blk, :, cols] + p1b[t, :, local]

    def rs_second_add(s):
        left, cols, local = piece(s)
        rs_wait(rs_r, 2, s)
        other = p2a[:, local] if left else p2b[:, local]
        total = acc[me, :, cols] + other
        hid[:, cols] = (hid[:, cols].astype(F32) + total).astype(BF16)

    def slab_in(l):
        return (pltpu.make_async_copy(k_slabs.at[l], k_slab.at[l], slab_sem.at[l, 0]),
                pltpu.make_async_copy(v_slabs.at[l], v_slab.at[l], slab_sem.at[l, 1]))

    def slab_out(l):
        return (pltpu.make_async_copy(k_slab.at[l], k_slabs_out.at[l], slab_sem.at[l, 2]),
                pltpu.make_async_copy(v_slab.at[l], v_slabs_out.at[l], slab_sem.at[l, 3]))

    def slab_fill(l):
        for c in slab_in(l):
            c.wait()
        row = lax.broadcasted_iota(jnp.int32, (SLAB, HEAD), 0)

        @pl.loop(0, GROUPS)
        def _(i):
            k8 = kn[al(i, GROUP), :]
            v8 = vn[al(i, GROUP), :]
            pos = pos_rep[al(i, GROUP * HEADS), :]
            for j in range(GROUP):
                q = i * GROUP + j
                hit = row == jnp.bitwise_and(pos[j * HEADS:j * HEADS + 1], SLAB - 1)
                k_slab[l, q] = jnp.where(hit, k8[j:j + 1], k_slab[l, q].astype(F32)).astype(BF16)
                v_slab[l, q] = jnp.where(hit, v8[j:j + 1], v_slab[l, q].astype(F32)).astype(BF16)

        for c in slab_out(l):
            c.start()

    order = range(len(PIECES))

    def hid_store(s):
        cols = pl.ds(*PIECES[s])
        return pltpu.make_async_copy(hid.at[:, cols], hid_out.at[:, cols], store_sem.at[s])

    def sends_over():
        gains_wait(gain_s)
        for l in range(LAYERS):
            for a in range(4):
                forwards_wait(fwd_s, l, a)
                relays_wait(rel_s, l, a)
            y_wait(l, y_s.at[l], 7 * ROWS)

        for l in range(LAYERS):
            for s in range(2):
                part = ffbuf[s].at[l, pl.ds(0, CHUNKS * (WAYS - 1) // WAYS)]
                pltpu.make_async_copy(part, part, chunk_s.at[l, s]).wait()

        for l in range(LAYERS):
            for c in slab_out(l):
                c.wait()

    for l in range(LAYERS):
        for c in slab_in(l):
            c.start()

    for c in loads:
        c.wait()

    for l in range(LAYERS):
        base = l * CHUNKS
        norm_into(hid, l, x_act, 0)
        if l == 0:
            for a in range(3):
                weights_relay_last(l, a)
        kv_start(l, 0, 0)
        for a in range(3):
            weights_arrived(l, a)
        tile_start(l, 0, 0, 0)

        @pl.loop(0, HEADS)
        def _(h, l=l):
            slot = lax.rem(h, 2)

            @pl.when(h + 1 < HEADS)
            def _():
                tile_start(l, 0, h + 1, 1 - slot)

            tile_wait(slot)
            q = rope(jnp.dot(x_act[...], w_tile[slot], preferred_element_type=F32))
            q_head[h] = (q * HEAD ** -0.5).astype(BF16).astype(F32)

        tile_start(l, 1, 0, 0)
        tile_start(l, 2, 0, 1)
        for h in range(HEADS):
            q_seq[:, h, :] = q_head[h]
        tile_wait(0)
        kn[...] = rope(jnp.dot(x_act[...], w_tile[0], preferred_element_type=F32)).astype(BF16).astype(F32)
        tile_wait(1)
        vn[...] = jnp.dot(x_act[...], w_tile[1], preferred_element_type=F32).astype(BF16).astype(F32)

        if l == 0:
            weights_relay_last(l, 3)
        else:
            unit_start(base + 2, 0)

        @pl.loop(0, GROUPS // 2)
        def _(i, l=l):
            attention_step(l, i)

        unit_start(base + 2, l)

        @pl.loop(GROUPS // 2, GROUPS)
        def _(i, l=l):
            attention_step(l, i)

        if l == 0:
            unit_start(base + 2, 1)
        for h in range(HEADS):
            a_flat[:, pl.ds(h * HEAD, HEAD)] = a_seq[:, h, :].astype(BF16)
        weights_arrived(l, 3)
        tile_start(l, 3, 0, 0)

        @pl.loop(0, HEADS)
        def _(n, l=l):
            slot = lax.rem(n, 2)

            @pl.when(n + 1 < HEADS)
            def _():
                tile_start(l, 3, n + 1, 1 - slot)

            tile_wait(slot)
            cols = al(n, HEAD)
            part = jnp.dot(a_flat[...], w_tile[slot], preferred_element_type=F32)
            hid[:, cols] = (hid[:, cols].astype(F32) + part).astype(BF16)

        norm_into(hid, LAYERS + l, y_full.at[l], me * ROWS)
        for m in (2, 4, 1):
            y_send(l, m).start()
        unit_start(base + 3, 0)
        for m in (2, 4):
            y_send(l, m).wait_recv()
            y_forward(l, m).start()
        unit_start(base + 3, 1)
        for m in (2, 4):
            y_relay(l, m).start()
        y_wait(l, y_r.at[l, 3], ROWS)
        y_relay(l, 6).start()
        y_wait(l, y_r.at[l, 0], 4 * ROWS)

        if l == 0:
            weights_start(1)

        @pl.loop(base + 4, base + CHUNKS - l)
        def _(g):
            unit_start(g, 0)
            unit_start(g, 1)

        if l == LAYERS - 1:
            unit_start(last_g, 0)
            last_up_start()

        def first_down():
            @pl.loop(0, D // SUB)
            def _(s):
                down_piece(al(s, SUB), True)

        def more_down():
            @pl.loop(0, D // SUB)
            def _(s):
                down_piece(al(s, SUB), False)

        tile_in(l, 0, 0)
        mlp_chunk(l, 0, False, first_down)

        @pl.loop(1, CHUNKS - 1)
        def _(k, l=l):
            mlp_chunk(l, k, False, more_down)

        if l == 0:
            for a in range(4):
                weights_relay_last(1, a)
            unit_start(CHUNKS, 0)

        def last_down():
            for s in order:
                down_piece(pl.ds(*PIECES[s]), False)
                for c in rs_core(s):
                    c.start()

        mlp_chunk(l, CHUNKS - 1, True, last_down)
        for s in order:
            rs_core_add(s)
            for c in rs_first(s):
                c.start()
        if l == 0:
            unit_start(CHUNKS, 1)
        slab_fill(l)
        if l == LAYERS - 1:
            sends_over()
        for s in order:
            rs_first_add(s)
            for c in rs_second(s):
                c.start()
        if l == 0:
            unit_start(CHUNKS + 1, 0)
            unit_start(CHUNKS + 1, 1)
        for s in order:
            rs_second_add(s)
            if l == LAYERS - 1:
                hid_store(s).start()
        if l == 0:
            for s in order:
                for phase in range(3):
                    rs_wait(rs_s, phase, s)

    for s in order:
        hid_store(s).wait()
        for phase in range(3):
            rs_wait(rs_s, phase, s)


def run_layers(*operands):
    any_spec = pl.BlockSpec(memory_space=pl.ANY)
    sds = jax.ShapeDtypeStruct
    dma = pltpu.SemaphoreType.DMA
    return pl.pallas_call(
        layers_kernel,
        name="layers",
        out_shape=[
            sds((ROWS, D), BF16), sds((LAYERS, ROWS, SLAB, HEAD), BF16), sds((LAYERS, ROWS, SLAB, HEAD), BF16),
            sds((LAYERS, WAYS, SHARD, D), BF16), sds((LAYERS, WAYS, SHARD, HEAD), BF16),
            sds((LAYERS, WAYS, SHARD, HEAD), BF16), sds((LAYERS, WAYS, SHARD, D), BF16),
            sds((LAYERS, CHUNKS, D, CHUNK), BF16), sds((LAYERS, CHUNKS, D, CHUNK), BF16),
        ],
        in_specs=[any_spec] * 24,
        out_specs=[any_spec] * 9,
        scratch_shapes=[
            pltpu.VMEM((WAYS, 8, SHARD), F32),
            pltpu.VMEM((ROWS, D), BF16),
            pltpu.VMEM((ROWS, D), BF16),
            pltpu.VMEM((HEADS, ROWS, HEAD), F32),
            pltpu.VMEM((ROWS, HEADS, HEAD), F32),
            pltpu.VMEM((ROWS, HEADS, HEAD), F32),
            pltpu.VMEM((ROWS, D), BF16),
            pltpu.VMEM((ROWS, HEAD), F32),
            pltpu.VMEM((ROWS, HEAD), F32),
            pltpu.VMEM((2, GROUP, SMAX, HEAD), BF16),
            pltpu.VMEM((2, GROUP, SMAX, HEAD), BF16),
            pltpu.VMEM((2, D, HEAD), BF16),
            pltpu.VMEM((LAYERS, BATCH, D), BF16),
            pltpu.VMEM((2, D, CHUNK), BF16),
            pltpu.VMEM((2, D, CHUNK), BF16),
            pltpu.VMEM((BATCH, CHUNK), F32),
            pltpu.VMEM((CHUNK, D), BF16),
            pltpu.VMEM((BATCH, CHUNK), BF16),
            pltpu.VMEM((WAYS, ROWS, D), F32),
            pltpu.VMEM((4, ROWS, D), F32),
            pltpu.VMEM((2, ROWS, D // 2), F32),
            pltpu.VMEM((2, ROWS, D // 2), F32),
            pltpu.VMEM((ROWS, D // 2), F32),
            pltpu.VMEM((ROWS, D // 2), F32),
            pltpu.VMEM((LAYERS, ROWS, SLAB, HEAD), BF16),
            pltpu.VMEM((LAYERS, ROWS, SLAB, HEAD), BF16),
            pltpu.VMEM((D, CHUNK), BF16),
            pltpu.VMEM((BATCH, 1), jnp.int32),
            pltpu.VMEM((ROWS, HALF), F32),
            pltpu.VMEM((ROWS, HALF), F32),
            dma((1,)), dma((1,)),
            dma((LAYERS, 4)), dma((LAYERS, 4)),
            dma((LAYERS, 4)), dma((LAYERS, 4)),
            dma((LAYERS, 2)), dma((LAYERS * CHUNKS, 2)),
            dma((LAYERS,)), dma((LAYERS, 4)),
            dma((3, len(PIECES))), dma((3, len(PIECES))),
            dma((2,)), dma((2, 2)), dma((2, 2)), dma((2,)), dma((LAYERS, 4)), dma((5,)), dma((len(PIECES),)),
        ],
        compiler_params=pltpu.CompilerParams(collective_id=0, has_side_effects=True, vmem_limit_bytes=63 * 2**20),
        cost_estimate=pl.CostEstimate(flops=60 * 10**9, bytes_accessed=300 * 10**6, transcendentals=0),
    )(*operands)


COPY_ROWS = 16


def slab_base(positions, s):
    return pl.multiple_of((positions[s] // SLAB) * SLAB, SLAB)


def copy_kernel(positions, k_in, v_in, k_out, v_out, k_slabs, v_slabs):
    k_out[...] = k_in[...]
    v_out[...] = v_in[...]
    first = pl.program_id(1) * COPY_ROWS
    for j in range(COPY_ROWS):
        base = slab_base(positions, first + j)
        k_slabs[0, j] = k_in[0, j, pl.ds(base, SLAB), :]
        v_slabs[0, j] = v_in[0, j, pl.ds(base, SLAB), :]


def copy_caches(positions, k_cache, v_cache):
    spec = pl.BlockSpec((1, COPY_ROWS, SMAX, HEAD), lambda l, i: (l, i, 0, 0))
    slab_spec = pl.BlockSpec((1, COPY_ROWS, SLAB, HEAD), lambda l, i: (l, i, 0, 0))
    shape = jax.ShapeDtypeStruct(k_cache.shape, k_cache.dtype)
    slab_shape = jax.ShapeDtypeStruct((LAYERS, ROWS, SLAB, HEAD), k_cache.dtype)
    return pl.pallas_call(
        copy_kernel, name="copy_caches", grid=(LAYERS, ROWS // COPY_ROWS),
        in_specs=[pl.BlockSpec(memory_space=pltpu.SMEM), spec, spec], out_specs=[spec, spec, slab_spec, slab_spec],
        out_shape=[shape, shape, slab_shape, slab_shape],
        compiler_params=pltpu.CompilerParams(vmem_limit_bytes=40 * 2**20),
        cost_estimate=pl.CostEstimate(flops=20 * 10**9, bytes_accessed=4 * k_cache.size * 2, transcendentals=0),
    )(positions, k_cache, v_cache)


def place_kernel(positions, hid_in, k_slabs, v_slabs, k_in, v_in, hid_out, k_out, v_out, hid, k_slab, v_slab, sems):
    def place(ref, s):
        return ref.at[:, s, pl.ds(slab_base(positions, s), SLAB), :]

    ins = [pltpu.make_async_copy(src.at[l], dst.at[l], sems.at[0, 2 * l + i])
           for l in range(LAYERS) for i, (src, dst) in enumerate(((k_slabs, k_slab), (v_slabs, v_slab)))]
    for c in ins:
        c.start()
    hid_load = pltpu.make_async_copy(hid_in, hid, sems.at[1, 2])
    hid_load.start()
    for c in ins:
        c.wait()

    @pl.loop(0, ROWS // 4)
    def _(i):
        for j in range(4):
            s = i * 4 + j
            pltpu.make_async_copy(k_slab.at[:, s], place(k_out, s), sems.at[1, 0]).start()
            pltpu.make_async_copy(v_slab.at[:, s], place(v_out, s), sems.at[1, 1]).start()

    hid_load.wait()
    hid_store = pltpu.make_async_copy(hid, hid_out, sems.at[1, 3])
    hid_store.start()
    pltpu.make_async_copy(k_slab, k_slab, sems.at[1, 0]).wait()
    pltpu.make_async_copy(v_slab, v_slab, sems.at[1, 1]).wait()
    hid_store.wait()


def place_rows(positions, hidden, k_slabs, v_slabs, k_copy, v_copy):
    any_spec = pl.BlockSpec(memory_space=pl.ANY)
    shape = jax.ShapeDtypeStruct(k_copy.shape, k_copy.dtype)
    slab = pltpu.VMEM((LAYERS, ROWS, SLAB, HEAD), BF16)
    return pl.pallas_call(
        place_kernel, name="place_rows",
        in_specs=[pl.BlockSpec(memory_space=pltpu.SMEM)] + [any_spec] * 5,
        out_specs=[any_spec] * 3, out_shape=[jax.ShapeDtypeStruct(hidden.shape, hidden.dtype), shape, shape], input_output_aliases={4: 1, 5: 2},
        scratch_shapes=[pltpu.VMEM((ROWS, D), BF16), slab, slab, pltpu.SemaphoreType.DMA((2, 4))],
        compiler_params=pltpu.CompilerParams(vmem_limit_bytes=63 * 2**20),
    )(positions, hidden, k_slabs, v_slabs, k_copy, v_copy)


def solution(mesh):
    batch_spec = P(("dp", "w"))
    cache_spec = P(None, ("dp", "w"))
    gain_spec = P(None, "w")
    weight_spec = P(None, "w", None)
    x_swap = [(s, s ^ 2) for s in range(WAYS)]
    y_swap = [(s, s ^ 4) for s in range(WAYS)]

    def per_device(hidden, positions, k_cache, v_cache, attn_norm, w_query, w_key, w_value, w_out, mlp_norm, w_gate, w_up, w_down):
        attn_weights = (w_query, w_key, w_value, w_out)
        from_x = tuple(lax.ppermute(w, "w", x_swap) for w in attn_weights)
        from_y = tuple(lax.ppermute(w, "w", y_swap) for w in attn_weights)
        cos_tab, sin_tab = rope_tables(positions)
        pos_rep = jnp.repeat(positions, HEADS)[:, None]
        gains = jnp.concatenate([attn_norm, mlp_norm, attn_norm, mlp_norm], axis=0)
        k_in, v_in, cos_tab, sin_tab, pos_rep, gains = lax.optimization_barrier((k_cache[:, :, 0], v_cache[:, :, 0], cos_tab, sin_tab, pos_rep, gains))
        k_copy, v_copy, k_slabs, v_slabs = copy_caches(positions, k_in, v_in)
        outs = run_layers(hidden, pos_rep, cos_tab, sin_tab, gains, k_copy, v_copy, k_slabs, v_slabs, *attn_weights, *from_x, *from_y, w_gate, w_up, w_down)
        hidden_out, k_out, v_out = place_rows(positions, outs[0], outs[1], outs[2], k_copy, v_copy)
        return hidden_out, k_out[:, :, None], v_out[:, :, None]

    in_specs = (batch_spec, batch_spec, cache_spec, cache_spec, gain_spec, weight_spec, weight_spec, weight_spec, weight_spec, gain_spec, weight_spec, weight_spec, weight_spec)
    out_specs = (batch_spec, cache_spec, cache_spec)
    return jax.shard_map(per_device, mesh=mesh, in_specs=in_specs, out_specs=out_specs, check_vma=False)
```
